32 devices in a mesh: horiz: 8 (over y, x, core), lev: 4 (over z).
Axes of the slice: x: 2, y: 2, z: 4, core: 2. Of those that a mesh axis runs over, the one named last changes fastest.
Arguments:
- source_state: bfloat16 [5, 68, 32768], P(None, 'lev', 'horiz'), may hold values from -6 to 6
- intersection: int32 [40], P('horiz'), may hold values from 0 to 7, as said below
- index_map: int32 [40, 512], P('horiz'), may hold values from 0 to 4095
- blocks: bfloat16 [40, 512, 2048], P('horiz'), may hold values from -0.125 to 0.125
- bracket: int32 [127, 16384], P(None, ('horiz', 'lev')), may hold values from 0 to 66
- fraction: float32 [127, 16384], P(None, ('horiz', 'lev')), may hold values from 0 to 1
Outputs:
- target_state: bfloat16 [5, 127, 16384], P(None, None, ('horiz', 'lev'))
The draws below stay inside these ranges and needn't reach their ends.
Inputs may be any that keep to these rules, and one draw needn't show every extreme that they name: For every target group g, intersection[g * 5] to intersection[g * 5 + 4] are the groups g - 2 to g + 2 modulo 8, each once, in some order.
All inputs are finite; a program needn't handle non-finite values.
Results may differ from the reference program's by a relative error of at most 0.0049.
Values may be sent and summed in bfloat16 or wider, within the bound.
A program may use at most 64 MiB of HBM per device.

```python
import jax
import jax.numpy as jnp
from jax import lax

F = 5
LEVELS_OUT = 127
R = 2
SRC_DEV = 4096
P_SIZE = 512
TGT_DEV = 2048
K = 5
GROUPS = 8
LEVELS_IN = 68
SRC_CELLS = 32768
TGT_CELLS = 16384
BLOCKS = 40


def draw_intersection(key, part):
    subkeys = jax.random.split(key, GROUPS)
    orders = jax.vmap(lambda subkey: jax.random.permutation(subkey, K))(subkeys)
    group_ids = jnp.arange(GROUPS, dtype=jnp.int32)[:, None]
    return ((group_ids + orders.astype(jnp.int32) - R) % GROUPS).reshape(-1).astype(jnp.int32)


def plant(drawn, key, least, high):
    extent = drawn.shape
    spot = [jax.random.randint(jax.random.fold_in(key, axis), (), 0, extent[axis]) for axis in range(len(extent))]
    drawn = drawn.at[tuple(spot)].set(least)
    longest = extent.index(max(extent))
    spot[longest] = (spot[longest] + 1) % extent[longest]
    return drawn.at[tuple(spot)].set(high)


def block_levels(key, extent, shards, smallest, top_value):
    def one(dim, parts):
        heights = jax.random.uniform(jax.random.fold_in(jax.random.fold_in(key, 6), dim), (parts,), jnp.float32, smallest / len(shards), top_value / len(shards))
        return jnp.repeat(jnp.exp(heights), extent[dim] // parts).reshape((-1,) + (1,) * (len(extent) - dim - 1))

    loudness = one(*shards[0])
    for cut in shards[1:]:
        loudness = loudness * one(*cut)
    return loudness


def scatter_about(key, dims, deviation, limit, pieces=(), held_as=jnp.bfloat16):
    array = jax.random.normal(key, dims, jnp.float32) * deviation
    if len(pieces) > 0:
        array = block_levels(key, dims, pieces, -0.22, 0.18) * array
    return jnp.clip(array, min=-limit, max=limit).astype(held_as)


def setup_inputs(seed: int = 0) -> dict:
    key_of = jax.random.split(jax.random.key(seed), 7)
    source_state = scatter_about(key_of[0], (F, LEVELS_IN, SRC_CELLS), 1.0, 6.0, ((1, 4), (2, 8)))
    intersection = draw_intersection(jax.random.fold_in(key_of[6], 71), 0)
    index_map = plant(jax.random.randint(key_of[2], (BLOCKS, P_SIZE), 0, SRC_DEV), jax.random.fold_in(key_of[2], 1), 0, SRC_DEV - 1).astype(jnp.int32)
    blocks = scatter_about(key_of[3], (BLOCKS, P_SIZE, TGT_DEV), (K * P_SIZE) ** -0.5, 0.125, ((0, 8),))
    bracket = plant(jax.random.randint(key_of[4], (LEVELS_OUT, TGT_CELLS), 0, LEVELS_IN - 1), jax.random.fold_in(key_of[4], 1), 0, (LEVELS_IN - 1) - 1).astype(jnp.int32)
    fraction = jnp.clip(1.0 * jax.random.uniform(key_of[5], (LEVELS_OUT, TGT_CELLS), jnp.float32) ** block_levels(key_of[5], (LEVELS_OUT, TGT_CELLS), ((1, 32),), -0.2, 0.2), 0.0, 1.0)
    return {"source_state": source_state, "intersection": intersection, "index_map": index_map, "blocks": blocks, "bracket": bracket, "fraction": fraction}


def reference(source_state, intersection, index_map, blocks, bracket, fraction):
    group_count = intersection.shape[0] // K
    fields_levels = F * LEVELS_IN
    source_tiles = jnp.transpose(source_state.reshape(fields_levels, group_count, SRC_DEV), (1, 0, 2))

    def remap_group(group_id):
        total_sum = jnp.zeros((fields_levels, TGT_DEV), jnp.float32)
        for block_slot in range(K):
            block_row = group_id * K + block_slot
            source_tile = source_tiles[intersection[block_row]]
            chosen = jnp.take(source_tile, index_map[block_row], axis=1).astype(jnp.float32)
            weights = blocks[block_row].astype(jnp.float32)
            total_sum = total_sum + jnp.dot(chosen, weights, preferred_element_type=jnp.float32)
        return total_sum.astype(jnp.bfloat16)

    remapped = lax.map(remap_group, jnp.arange(group_count, dtype=jnp.int32))
    horizontal = jnp.transpose(remapped, (1, 0, 2)).reshape(F, LEVELS_IN, group_count * TGT_DEV)
    widened = horizontal.astype(jnp.float32)
    below_level = jnp.take_along_axis(widened, bracket[None], axis=1)
    above_level = jnp.take_along_axis(widened, bracket[None] + 1, axis=1)
    upper_share = fraction[None]
    return ((1.0 - upper_share) * below_level + upper_share * above_level).astype(jnp.bfloat16)
```

```python
import functools

import jax
import jax.numpy as jnp
from jax import lax
from jax.experimental import pallas as pl
from jax.experimental.pallas import tpu as pltpu
from jax.sharding import PartitionSpec as P

MESH = pl.DeviceIdType.MESH
HIGH = 256
LANES = 128


def round_up(value, step):
    return (value + step - 1) // step * step


def row_plan(fields, slab_levels):
    whole = slab_levels // 16 * 16
    rest = slab_levels - whole
    extra = round_up(fields * rest, 8)
    base = round_up(extra, 16)
    return whole, rest, extra, base, base + fields * whole


def field_groups(fields):
    first = max(1, fields // 5)
    second = (fields - first + 1) // 2
    cuts = [0, first, first + second, fields]
    return [(a, b) for a, b in zip(cuts[:-1], cuts[1:]) if b > a]


def rows_at(table, index):
    numbers = lax.GatherDimensionNumbers(
        offset_dims=(),
        collapsed_slice_dims=(0,),
        start_index_map=(0,),
        operand_batching_dims=(1,),
        start_indices_batching_dims=(1,),
    )
    return lax.gather(
        table, index[..., None], numbers, slice_sizes=(1, 1), mode=lax.GatherScatterMode.PROMISE_IN_BOUNDS
    )


def regrid_kernel(
    groups, levs, depth,
    inter_hbm, index_hbm, source_hbm, blocks_hbm, bracket_hbm, fraction_hbm, out_ref,
    inter_ref, index_ref, tile, spare, stack, weights, request, wanted, chosen, arrived, total, slab, got,
    brackets, fractions, raw, table,
    inter_sem, index_sem, tile_sem, weight_sem, bracket_sem, fraction_sem,
    req_send, req_recv, val_send, val_recv, lev_send, lev_recv,
):
    fields, slab_levels, cells = tile.shape
    whole, rest, extra, base, rows = row_plan(fields, slab_levels)
    count = 2 * depth + 1
    wide = index_ref.shape[1]
    me = lax.axis_index("horiz")
    my_lev = lax.axis_index("lev")
    levels_out, columns = brackets.shape
    plan = field_groups(fields)
    chunks = [(base + a * whole, (b - a) * whole) for a, b in plan]
    parts = [[i] for i in range(len(chunks))]
    spans = list(chunks)
    if extra:
        parts[0].append(len(chunks))
        spans[0] = (0, base + chunks[0][1])
        chunks.append((0, extra))

    barrier = pltpu.get_barrier_semaphore()
    offsets = [o for o in range(-depth, depth + 1) if o != 0]
    for offset in offsets:
        pl.semaphore_signal(
            barrier, inc=1, device_id={"horiz": lax.rem(me + offset + groups, groups)}, device_id_type=MESH
        )
    for hop in range(1, levs):
        pl.semaphore_signal(
            barrier, inc=1, device_id={"lev": lax.rem(my_lev + hop, levs)}, device_id_type=MESH
        )

    inter_copy = pltpu.make_async_copy(inter_hbm, inter_ref, inter_sem)
    inter_copy.start()
    index_copy = pltpu.make_async_copy(index_hbm, index_ref, index_sem)
    index_copy.start()
    tile_copy = pltpu.make_async_copy(source_hbm, tile, tile_sem)
    tile_copy.start()
    inter_copy.wait()
    index_copy.wait()
    slots = []
    for place in range(count):
        group = lax.rem(me + place - depth + groups, groups)
        cells_wanted = jnp.zeros((1, wide), jnp.int32)
        slot = jnp.int32(0)
        for k in range(count):
            hit = (inter_ref[k] == group).astype(jnp.int32)
            cells_wanted = cells_wanted + index_ref[k : k + 1, :] * hit
            slot = jnp.where(inter_ref[k] == group, jnp.int32(k), slot)
        slots.append(slot)
        if place == depth:
            wanted[place] = cells_wanted
        else:
            request[place] = cells_wanted

    tile_copy.wait()
    weight_copies = []
    for part in range(levs):
        copy = pltpu.make_async_copy(
            blocks_hbm.at[:, :, pl.ds(part * columns, columns)], weights.at[:, part], weight_sem.at[part]
        )
        copy.start()
        weight_copies.append(copy)
    bracket_copy = pltpu.make_async_copy(bracket_hbm, brackets, bracket_sem)
    bracket_copy.start()
    fraction_copy = pltpu.make_async_copy(fraction_hbm, fractions, fraction_sem)
    fraction_copy.start()
    blocks_high = cells // HIGH
    if base:
        spare[...] = jnp.zeros(spare.shape, jnp.float32)
        for field in range(fields):
            if rest:
                spare[pl.ds(field * rest, rest), :] = tile[field, pl.ds(whole, rest), :].astype(jnp.float32)
    for chunk in range(blocks_high):
        lane = pl.ds(chunk * HIGH, HIGH)
        if base:
            stack[pl.ds(chunk * rows, base), :] = spare[:, lane].astype(jnp.bfloat16)
        for field in range(fields):
            stack[pl.ds(chunk * rows + base + field * whole, whole), :] = tile[field, pl.ds(0, whole), lane]

    def request_copy(place):
        return pltpu.make_async_remote_copy(
            src_ref=request.at[place],
            dst_ref=wanted.at[2 * depth - place],
            send_sem=req_send.at[place],
            recv_sem=req_recv.at[2 * depth - place],
            device_id={"horiz": lax.rem(me + place - depth + groups, groups)},
            device_id_type=MESH,
        )

    def value_copy(place, piece):
        first, size = chunks[piece]
        return pltpu.make_async_remote_copy(
            src_ref=chosen.at[place, pl.ds(first, size)],
            dst_ref=arrived.at[2 * depth - place, pl.ds(first, size)],
            send_sem=val_send.at[piece, place],
            recv_sem=val_recv.at[piece, 2 * depth - place],
            device_id={"horiz": lax.rem(me + place - depth + groups, groups)},
            device_id_type=MESH,
        )

    def lev_copy(hop, piece):
        block = pl.ds(*chunks[piece])
        return pltpu.make_async_remote_copy(
            src_ref=slab.at[hop, block],
            dst_ref=got.at[my_lev, block],
            send_sem=lev_send.at[piece, hop],
            recv_sem=lev_recv.at[piece, hop],
            device_id={"lev": lax.rem(my_lev + hop, levs)},
            device_id_type=MESH,
        )

    pl.semaphore_wait(barrier, len(offsets) + levs - 1)
    for reach in range(depth, 0, -1):
        request_copy(depth - reach).start()
        request_copy(depth + reach).start()

    ids = lax.broadcasted_iota(jnp.int32, (HIGH, 1), 0).astype(jnp.float32).astype(jnp.bfloat16)

    def select(place):
        cell = wanted[place]
        high = cell // HIGH
        low = (cell - high * HIGH).astype(jnp.float32).astype(jnp.bfloat16)
        picker = jnp.where(ids == low, jnp.bfloat16(1), jnp.bfloat16(0))
        found = jnp.dot(stack[...], picker, preferred_element_type=jnp.float32)
        values = jnp.zeros((rows, wide), jnp.float32)
        for chunk in range(blocks_high):
            values = jnp.where(high == chunk, found[chunk * rows : (chunk + 1) * rows], values)
        return values.astype(jnp.bfloat16)

    arrived[depth] = select(depth)

    lean = 1 - 2 * (me % 2)

    def order_place(step):
        reach = depth - step // 2
        return depth + reach * (2 * (step % 2) - 1) * lean

    def serve(step, carry):
        place = order_place(step)
        request_copy(2 * depth - place).wait_recv()
        chosen[place] = select(place)
        for piece in parts[0]:
            value_copy(place, piece).start()
        return carry

    last = 2 * depth - 1
    lax.fori_loop(0, last, serve, 0)
    for later in range(1, len(parts)):
        for step in range(last):
            for piece in parts[later]:
                value_copy(order_place(step), piece).start()
    near = order_place(last)
    request_copy(2 * depth - near).wait_recv()
    chosen[near] = select(near)
    for piece in range(len(chunks)):
        value_copy(near, piece).start()

    for copy in weight_copies:
        copy.wait()

    def slot_of(place):
        slot = slots[0]
        for k in range(1, count):
            slot = jnp.where(place == k, slots[k], slot)
        return slot

    values = arrived[depth]
    for part in range(levs):
        total[part] = jnp.dot(values, weights[slots[depth], part], preferred_element_type=jnp.float32)
    for piece in range(len(chunks)):
        value_copy(2 * depth - near, piece).wait_recv()
    values = arrived[near]
    near_slot = slot_of(near)
    for part in range(levs):
        total[part] += jnp.dot(values, weights[near_slot, part], preferred_element_type=jnp.float32)

    for number in range(len(parts)):
        block = pl.ds(*spans[number])
        for step in range(last):
            place = order_place(step)
            slot = slot_of(place)
            for piece in parts[number]:
                value_copy(2 * depth - place, piece).wait_recv()
            values = arrived[place, block]
            for hop in list(range(1, levs)) + [0]:
                part = lax.rem(my_lev + hop, levs)
                term = jnp.dot(values, weights[slot, part], preferred_element_type=jnp.float32)
                if step < last - 1:
                    total[part, block] += term
                elif hop:
                    slab[hop, block] = (total[part, block] + term).astype(jnp.bfloat16)
                    for piece in parts[number]:
                        lev_copy(hop, piece).start()
                else:
                    got[my_lev, block] = (total[part, block] + term).astype(jnp.bfloat16)

    bracket_copy.wait()
    fraction_copy.wait()
    levels_in = levs * slab_levels
    step_rows = 16
    table[:, pl.ds(levels_in, table.shape[1] - levels_in), :] = jnp.zeros(
        (table.shape[0], table.shape[1] - levels_in, LANES), jnp.float32
    )

    def interpolate(first, end):
        held = list(range(first, end))

        def work(strip, carry):
            lane = pl.ds(pl.multiple_of(strip * LANES, LANES), LANES)
            for lev in range(levs):
                if rest:
                    raw[lev] = got[lev, pl.ds(0, base), lane].astype(jnp.float32)
                for place, field in enumerate(held):
                    table[place, pl.ds(lev * slab_levels, whole), :] = got[
                        lev, pl.ds(base + field * whole, whole), lane
                    ].astype(jnp.float32)
                    if rest:
                        table[place, pl.ds(lev * slab_levels + whole, rest), :] = raw[
                            lev, pl.ds(field * rest, rest), :
                        ]
            for start in range(0, levels_out, step_rows):
                size = min(step_rows, levels_out - start)
                bracket = brackets[start : start + size, lane]
                upper = fractions[start : start + size, lane]
                if size < step_rows:
                    bracket = jnp.concatenate([bracket, jnp.zeros((step_rows - size, LANES), jnp.int32)], axis=0)
                    upper = jnp.concatenate([upper, jnp.zeros((step_rows - size, LANES), jnp.float32)], axis=0)
                halves = [bracket[i : i + 8] for i in range(0, step_rows, 8)]
                high = [half >> 3 for half in halves]
                low = [half & 7 for half in halves]
                below = [[jnp.zeros((8, LANES), jnp.float32) for _ in halves] for _ in held]
                above = [[jnp.zeros((8, LANES), jnp.float32) for _ in halves] for _ in held]
                for group in range((levels_in - 2) // 8 + 1):
                    masks = [h == group for h in high]
                    for place in range(len(held)):
                        here = table[place, pl.ds(group * 8, 8), :]
                        over = table[place, pl.ds(group * 8 + 1, 8), :]
                        for i, mask in enumerate(masks):
                            below[place][i] = jnp.where(mask, rows_at(here, low[i]), below[place][i])
                            above[place][i] = jnp.where(mask, rows_at(over, low[i]), above[place][i])
                for place, field in enumerate(held):
                    mixed = (1.0 - upper) * jnp.concatenate(below[place], axis=0) + upper * jnp.concatenate(
                        above[place], axis=0
                    )
                    out_ref[field, start : start + size, lane] = mixed[:size].astype(jnp.bfloat16)
            return carry

        lax.fori_loop(0, columns // LANES, work, 0)

    for number, (first, end) in enumerate(plan):
        for hop in range(1, levs):
            for piece in parts[number]:
                lev_copy(hop, piece).wait_recv()
        interpolate(first, end)

    for piece in range(len(chunks)):
        for hop in range(1, levs):
            lev_copy(hop, piece).wait_send()
        for offset in offsets:
            value_copy(depth + offset, piece).wait_send()
    for offset in offsets:
        request_copy(depth + offset).wait_send()


def store_kernel(held_ref, out_hbm, sem):
    copies = [
        pltpu.make_async_copy(held_ref.at[field], out_hbm.at[field], sem.at[field])
        for field in range(held_ref.shape[0])
    ]
    for copy in copies:
        copy.start()
    for copy in copies:
        copy.wait()


def local(levs, groups, source_state, intersection, index_map, blocks, bracket, fraction):
    fields, slab_levels, cells = source_state.shape
    count, wide, targets = blocks.shape
    depth = (count - 1) // 2
    whole, rest, extra, base, rows = row_plan(fields, slab_levels)
    columns = targets // levs
    levels_out = bracket.shape[0]
    plan = field_groups(fields)
    pieces = len(plan) + (1 if extra else 0)
    most = max(b - a for a, b in plan)
    bf16, f32, i32 = jnp.bfloat16, jnp.float32, jnp.int32
    dma = pltpu.SemaphoreType.DMA
    held = pl.pallas_call(
        functools.partial(regrid_kernel, groups, levs, depth),
        name="regrid",
        out_shape=pltpu.VMEM((fields, levels_out, columns), bf16),
        in_specs=[pl.BlockSpec(memory_space=pltpu.HBM)] * 6,
        out_specs=pl.BlockSpec(memory_space=pltpu.VMEM),
        scratch_shapes=[
            pltpu.SMEM((count,), i32),
            pltpu.VMEM((count, wide), i32),
            pltpu.VMEM((fields, slab_levels, cells), bf16),
            pltpu.VMEM((max(base, 8), cells), f32),
            pltpu.VMEM((cells // HIGH * rows, HIGH), bf16),
            pltpu.VMEM((count, levs, wide, columns), bf16),
            pltpu.VMEM((count, 1, wide), i32),
            pltpu.VMEM((count, 1, wide), i32),
            pltpu.VMEM((count, rows, wide), bf16),
            pltpu.VMEM((count, rows, wide), bf16),
            pltpu.VMEM((levs, rows, columns), f32),
            pltpu.VMEM((levs, rows, columns), bf16),
            pltpu.VMEM((levs, rows, columns), bf16),
            pltpu.VMEM((levels_out, columns), i32),
            pltpu.VMEM((levels_out, columns), f32),
            pltpu.VMEM((levs, max(base, 8), LANES), f32),
            pltpu.VMEM((most, round_up(levs * slab_levels, 8) + 8, LANES), f32),
            dma,
            dma,
            dma,
            dma((levs,)),
            dma,
            dma,
            dma((count,)),
            dma((count,)),
            dma((pieces, count)),
            dma((pieces, count)),
            dma((pieces, levs)),
            dma((pieces, levs)),
        ],
        compiler_params=pltpu.CompilerParams(
            collective_id=0, has_side_effects=True, vmem_limit_bytes=56 * 1024 * 1024
        ),
        cost_estimate=pl.CostEstimate(
            flops=2 * rows * count * wide * (cells + targets),
            bytes_accessed=2 * blocks.size + 2 * source_state.size,
            transcendentals=0,
        ),
    )(intersection, index_map, source_state, blocks, bracket, fraction)
    return pl.pallas_call(
        store_kernel,
        name="store",
        out_shape=jax.ShapeDtypeStruct(held.shape, bf16),
        in_specs=[pl.BlockSpec(memory_space=pltpu.VMEM)],
        out_specs=pl.BlockSpec(memory_space=pltpu.HBM),
        scratch_shapes=[dma((fields,))],
        compiler_params=pltpu.CompilerParams(vmem_limit_bytes=8 * 1024 * 1024),
    )(held)


def solution(mesh):
    in_specs = (
        P(None, "lev", "horiz"),
        P("horiz"),
        P("horiz", None),
        P("horiz", None, None),
        P(None, ("horiz", "lev")),
        P(None, ("horiz", "lev")),
    )
    out_specs = P(None, None, ("horiz", "lev"))
    body = functools.partial(local, mesh.shape["lev"], mesh.shape["horiz"])
    return jax.shard_map(body, mesh=mesh, in_specs=in_specs, out_specs=out_specs, check_vma=False)
```

```python
import functools

import jax
import jax.numpy as jnp
from jax import lax
from jax.experimental import pallas as pl
from jax.experimental.pallas import tpu as pltpu
from jax.sharding import PartitionSpec as P

MESH = pl.DeviceIdType.MESH
HIGH = 256
LANES = 128


def round_up(value, step):
    return (value + step - 1) // step * step


def row_plan(fields, slab_levels):
    whole = slab_levels // 16 * 16
    rest = slab_levels - whole
    extra = round_up(fields * rest, 8)
    base = round_up(extra, 16)
    return whole, rest, extra, base, base + fields * whole


def field_groups(fields):
    first = max(1, fields // 5)
    second = (fields - first + 1) // 2
    cuts = [0, first, first + second, fields]
    return [(a, b) for a, b in zip(cuts[:-1], cuts[1:]) if b > a]


def rows_at(table, index):
    numbers = lax.GatherDimensionNumbers(
        offset_dims=(),
        collapsed_slice_dims=(0,),
        start_index_map=(0,),
        operand_batching_dims=(1,),
        start_indices_batching_dims=(1,),
    )
    return lax.gather(
        table, index[..., None], numbers, slice_sizes=(1, 1), mode=lax.GatherScatterMode.PROMISE_IN_BOUNDS
    )


def regrid_kernel(
    groups, levs, depth,
    inter_hbm, index_hbm, source_hbm, blocks_hbm, bracket_hbm, fraction_hbm, out_ref,
    inter_ref, index_ref, tile, spare, first_rows, other_rows, weights, request, wanted, chosen, arrived, total, slab, got,
    brackets, fractions, raw, table,
    inter_sem, index_sem, tile_sem, weight_sem, bracket_sem, fraction_sem,
    req_send, req_recv, val_send, val_recv, lev_send, lev_recv,
):
    fields, slab_levels, cells = tile.shape
    whole, rest, extra, base, rows = row_plan(fields, slab_levels)
    count = 2 * depth + 1
    wide = index_ref.shape[1]
    me = lax.axis_index("horiz")
    my_lev = lax.axis_index("lev")
    levels_out, columns = brackets.shape
    plan = field_groups(fields)
    chunks = [(base + a * whole, (b - a) * whole) for a, b in plan]
    parts = [[i] for i in range(len(chunks))]
    spans = list(chunks)
    if extra:
        parts[0].append(len(chunks))
        spans[0] = (0, base + chunks[0][1])
        chunks.append((0, extra))

    barrier = pltpu.get_barrier_semaphore()
    offsets = [o for o in range(-depth, depth + 1) if o != 0]
    for offset in offsets:
        pl.semaphore_signal(
            barrier, inc=1, device_id={"horiz": lax.rem(me + offset + groups, groups)}, device_id_type=MESH
        )
    for hop in range(1, levs):
        pl.semaphore_signal(
            barrier, inc=1, device_id={"lev": lax.rem(my_lev + hop, levs)}, device_id_type=MESH
        )

    inter_copy = pltpu.make_async_copy(inter_hbm, inter_ref, inter_sem)
    inter_copy.start()
    index_copy = pltpu.make_async_copy(index_hbm, index_ref, index_sem)
    index_copy.start()
    tile_copy = pltpu.make_async_copy(source_hbm, tile, tile_sem)
    tile_copy.start()
    weight_copies = []
    for part in range(levs):
        copy = pltpu.make_async_copy(
            blocks_hbm.at[:, :, pl.ds(part * columns, columns)], weights.at[:, part], weight_sem.at[part]
        )
        copy.start()
        weight_copies.append(copy)
    bracket_copy = pltpu.make_async_copy(bracket_hbm, brackets, bracket_sem)
    bracket_copy.start()
    fraction_copy = pltpu.make_async_copy(fraction_hbm, fractions, fraction_sem)
    fraction_copy.start()
    inter_copy.wait()
    index_copy.wait()
    slots = []
    for place in range(count):
        group = lax.rem(me + place - depth + groups, groups)
        cells_wanted = jnp.zeros((1, wide), jnp.int32)
        slot = jnp.int32(0)
        for k in range(count):
            hit = (inter_ref[k] == group).astype(jnp.int32)
            cells_wanted = cells_wanted + index_ref[k : k + 1, :] * hit
            slot = jnp.where(inter_ref[k] == group, jnp.int32(k), slot)
        slots.append(slot)
        if place == depth:
            wanted[place] = cells_wanted
        else:
            request[place] = cells_wanted

    def request_copy(place):
        return pltpu.make_async_remote_copy(
            src_ref=request.at[place],
            dst_ref=wanted.at[2 * depth - place],
            send_sem=req_send.at[place],
            recv_sem=req_recv.at[2 * depth - place],
            device_id={"horiz": lax.rem(me + place - depth + groups, groups)},
            device_id_type=MESH,
        )

    def value_copy(place, piece):
        first, size = chunks[piece]
        return pltpu.make_async_remote_copy(
            src_ref=chosen.at[place, pl.ds(first, size)],
            dst_ref=arrived.at[2 * depth - place, pl.ds(first, size)],
            send_sem=val_send.at[piece, place],
            recv_sem=val_recv.at[piece, 2 * depth - place],
            device_id={"horiz": lax.rem(me + place - depth + groups, groups)},
            device_id_type=MESH,
        )

    def dest_of(turn):
        return turn + (turn >= my_lev).astype(jnp.int32)

    def lev_copy(turn, piece):
        block = pl.ds(*chunks[piece])
        return pltpu.make_async_remote_copy(
            src_ref=slab.at[turn, block],
            dst_ref=got.at[my_lev, block],
            send_sem=lev_send.at[piece, turn],
            recv_sem=lev_recv.at[piece, my_lev],
            device_id={"lev": dest_of(turn)},
            device_id_type=MESH,
        )

    def lev_arrival(turn, piece):
        block = pl.ds(*chunks[piece])
        sender = dest_of(turn)
        return pltpu.make_async_remote_copy(
            src_ref=slab.at[turn, block],
            dst_ref=got.at[sender, block],
            send_sem=lev_send.at[piece, turn],
            recv_sem=lev_recv.at[piece, sender],
            device_id={"lev": sender},
            device_id_type=MESH,
        )

    pl.semaphore_wait(barrier, len(offsets) + levs - 1)
    for reach in range(depth, 0, -1):
        request_copy(depth - reach).start()
        request_copy(depth + reach).start()

    tile_copy.wait()
    high_count = cells // HIGH
    head = spans[0][1]
    tail = rows - head
    if base:
        spare[...] = jnp.zeros(spare.shape, jnp.float32)
        for field in range(fields):
            if rest:
                spare[pl.ds(field * rest, rest), :] = tile[field, pl.ds(whole, rest), :].astype(jnp.float32)
    for chunk in range(high_count):
        lane = pl.ds(chunk * HIGH, HIGH)
        if base:
            first_rows[pl.ds(chunk * head, base), :] = spare[:, lane].astype(jnp.bfloat16)
        for field in range(fields):
            if field < plan[0][1]:
                spot = first_rows.at[pl.ds(chunk * head + base + field * whole, whole)]
            else:
                spot = other_rows.at[pl.ds(chunk * tail + base + field * whole - head, whole)]
            spot[...] = tile[field, pl.ds(0, whole), lane]

    ids = lax.broadcasted_iota(jnp.int32, (HIGH, 1), 0).astype(jnp.float32).astype(jnp.bfloat16)

    def select(place, held):
        cell = wanted[place]
        high = cell // HIGH
        low = (cell - high * HIGH).astype(jnp.float32).astype(jnp.bfloat16)
        picker = jnp.where(ids == low, jnp.bfloat16(1), jnp.bfloat16(0))
        found = jnp.dot(held[...], picker, preferred_element_type=jnp.float32)
        size = held.shape[0] // high_count
        values = jnp.zeros((size, wide), jnp.float32)
        for chunk in range(high_count):
            values = jnp.where(high == chunk, found[chunk * size : (chunk + 1) * size], values)
        return values.astype(jnp.bfloat16)

    first_span, other_span = pl.ds(0, head), pl.ds(head, tail)
    arrived[depth, first_span] = select(depth, first_rows)
    arrived[depth, other_span] = select(depth, other_rows)

    lean = 1 - 2 * (me % 2)

    def order_place(step):
        reach = depth - step // 2
        return depth + reach * (2 * (step % 2) - 1) * lean

    last = 2 * depth - 1

    def serve(step, carry):
        place = order_place(step)
        request_copy(2 * depth - place).wait_recv()
        chosen[place, first_span] = select(place, first_rows)
        for piece in parts[0]:
            value_copy(place, piece).start()
        return carry

    lax.fori_loop(0, last, serve, 0)

    def serve_rest(step, carry):
        place = order_place(step)
        chosen[place, other_span] = select(place, other_rows)
        for piece in parts[1]:
            value_copy(place, piece).start()
        return carry

    lax.fori_loop(0, last, serve_rest, 0)
    for later in range(2, len(parts)):
        for step in range(last):
            for piece in parts[later]:
                value_copy(order_place(step), piece).start()
    near = order_place(last)
    request_copy(2 * depth - near).wait_recv()
    chosen[near, first_span] = select(near, first_rows)
    chosen[near, other_span] = select(near, other_rows)
    for piece in range(len(chunks)):
        value_copy(near, piece).start()

    for copy in weight_copies:
        copy.wait()

    def slot_of(place):
        slot = slots[0]
        for k in range(1, count):
            slot = jnp.where(place == k, slots[k], slot)
        return slot

    values = arrived[depth]
    for part in range(levs):
        total[part] = jnp.dot(values, weights[slots[depth], part], preferred_element_type=jnp.float32)
    for piece in range(len(chunks)):
        value_copy(2 * depth - near, piece).wait_recv()
    values = arrived[near]
    near_slot = slot_of(near)
    for part in range(levs):
        total[part] += jnp.dot(values, weights[near_slot, part], preferred_element_type=jnp.float32)

    def send_others(number):
        for turn in range(1, levs - 1):
            for piece in parts[number]:
                lev_copy(turn, piece).start()

    far = [order_place(step) for step in range(last)]
    far_slots = [slot_of(place) for place in far]
    for number in range(len(parts)):
        block = pl.ds(*spans[number])
        for place in far:
            for piece in parts[number]:
                value_copy(2 * depth - place, piece).wait_recv()
        values = [arrived[place, block] for place in far]

        def column_sum(part):
            sums = total[part, block]
            for value, slot in zip(values, far_slots):
                sums += jnp.dot(value, weights[slot, part], preferred_element_type=jnp.float32)
            return sums.astype(jnp.bfloat16)

        slab[0, block] = column_sum(dest_of(0))
        for piece in parts[number]:
            lev_copy(0, piece).start()
        if number == len(parts) - 1:
            send_others(number - 1)
        for turn in range(1, levs - 1):
            slab[turn, block] = column_sum(dest_of(turn))
        if number != len(parts) - 2:
            send_others(number)
        got[my_lev, block] = column_sum(my_lev)

    bracket_copy.wait()
    fraction_copy.wait()
    levels_in = levs * slab_levels
    step_rows = 16
    table[:, pl.ds(levels_in, table.shape[1] - levels_in), :] = jnp.zeros(
        (table.shape[0], table.shape[1] - levels_in, LANES), jnp.float32
    )

    def interpolate(first, end):
        held = list(range(first, end))

        def work(strip, carry):
            lane = pl.ds(pl.multiple_of(strip * LANES, LANES), LANES)
            for lev in range(levs):
                if rest:
                    raw[lev] = got[lev, pl.ds(0, base), lane].astype(jnp.float32)
                for place, field in enumerate(held):
                    table[place, pl.ds(lev * slab_levels, whole), :] = got[
                        lev, pl.ds(base + field * whole, whole), lane
                    ].astype(jnp.float32)
                    if rest:
                        table[place, pl.ds(lev * slab_levels + whole, rest), :] = raw[
                            lev, pl.ds(field * rest, rest), :
                        ]
            for start in range(0, levels_out, step_rows):
                size = min(step_rows, levels_out - start)
                bracket = brackets[start : start + size, lane]
                upper = fractions[start : start + size, lane]
                if size < step_rows:
                    bracket = jnp.concatenate([bracket, jnp.zeros((step_rows - size, LANES), jnp.int32)], axis=0)
                    upper = jnp.concatenate([upper, jnp.zeros((step_rows - size, LANES), jnp.float32)], axis=0)
                halves = [bracket[i : i + 8] for i in range(0, step_rows, 8)]
                high = [half >> 3 for half in halves]
                low = [half & 7 for half in halves]
                below = [[jnp.zeros((8, LANES), jnp.float32) for _ in halves] for _ in held]
                above = [[jnp.zeros((8, LANES), jnp.float32) for _ in halves] for _ in held]
                for group in range((levels_in - 2) // 8 + 1):
                    masks = [h == group for h in high]
                    for place in range(len(held)):
                        here = table[place, pl.ds(group * 8, 8), :]
                        over = table[place, pl.ds(group * 8 + 1, 8), :]
                        for i, mask in enumerate(masks):
                            below[place][i] = jnp.where(mask, rows_at(here, low[i]), below[place][i])
                            above[place][i] = jnp.where(mask, rows_at(over, low[i]), above[place][i])
                for place, field in enumerate(held):
                    mixed = (1.0 - upper) * jnp.concatenate(below[place], axis=0) + upper * jnp.concatenate(
                        above[place], axis=0
                    )
                    out_ref[field, start : start + size, lane] = mixed[:size].astype(jnp.bfloat16)
            return carry

        lax.fori_loop(0, columns // LANES, work, 0)

    for number, (first, end) in enumerate(plan):
        for turn in range(levs - 1):
            for piece in parts[number]:
                lev_arrival(turn, piece).wait_recv()
        interpolate(first, end)

    for piece in range(len(chunks)):
        for turn in range(levs - 1):
            lev_copy(turn, piece).wait_send()
        for offset in offsets:
            value_copy(depth + offset, piece).wait_send()
    for offset in offsets:
        request_copy(depth + offset).wait_send()


def store_kernel(held_ref, out_hbm, sem):
    copies = [
        pltpu.make_async_copy(held_ref.at[field], out_hbm.at[field], sem.at[field])
        for field in range(held_ref.shape[0])
    ]
    for copy in copies:
        copy.start()
    for copy in copies:
        copy.wait()


def local(levs, groups, source_state, intersection, index_map, blocks, bracket, fraction):
    fields, slab_levels, cells = source_state.shape
    count, wide, targets = blocks.shape
    depth = (count - 1) // 2
    whole, rest, extra, base, rows = row_plan(fields, slab_levels)
    columns = targets // levs
    levels_out = bracket.shape[0]
    plan = field_groups(fields)
    pieces = len(plan) + (1 if extra else 0)
    most = max(b - a for a, b in plan)
    head = base + plan[0][1] * whole
    bf16, f32, i32 = jnp.bfloat16, jnp.float32, jnp.int32
    dma = pltpu.SemaphoreType.DMA
    held = pl.pallas_call(
        functools.partial(regrid_kernel, groups, levs, depth),
        name="regrid",
        out_shape=pltpu.VMEM((fields, levels_out, columns), bf16),
        in_specs=[pl.BlockSpec(memory_space=pltpu.HBM)] * 6,
        out_specs=pl.BlockSpec(memory_space=pltpu.VMEM),
        scratch_shapes=[
            pltpu.SMEM((count,), i32),
            pltpu.VMEM((count, wide), i32),
            pltpu.VMEM((fields, slab_levels, cells), bf16),
            pltpu.VMEM((max(base, 8), cells), f32),
            pltpu.VMEM((cells // HIGH * head, HIGH), bf16),
            pltpu.VMEM((cells // HIGH * (rows - head), HIGH), bf16),
            pltpu.VMEM((count, levs, wide, columns), bf16),
            pltpu.VMEM((count, 1, wide), i32),
            pltpu.VMEM((count, 1, wide), i32),
            pltpu.VMEM((count, rows, wide), bf16),
            pltpu.VMEM((count, rows, wide), bf16),
            pltpu.VMEM((levs, rows, columns), f32),
            pltpu.VMEM((levs, rows, columns), bf16),
            pltpu.VMEM((levs, rows, columns), bf16),
            pltpu.VMEM((levels_out, columns), i32),
            pltpu.VMEM((levels_out, columns), f32),
            pltpu.VMEM((levs, max(base, 8), LANES), f32),
            pltpu.VMEM((most, round_up(levs * slab_levels, 8) + 8, LANES), f32),
            dma,
            dma,
            dma,
            dma((levs,)),
            dma,
            dma,
            dma((count,)),
            dma((count,)),
            dma((pieces, count)),
            dma((pieces, count)),
            dma((pieces, levs)),
            dma((pieces, levs)),
        ],
        compiler_params=pltpu.CompilerParams(
            collective_id=0, has_side_effects=True, vmem_limit_bytes=56 * 1024 * 1024
        ),
        cost_estimate=pl.CostEstimate(
            flops=2 * rows * count * wide * (cells + targets),
            bytes_accessed=2 * blocks.size + 2 * source_state.size,
            transcendentals=0,
        ),
    )(intersection, index_map, source_state, blocks, bracket, fraction)
    return pl.pallas_call(
        store_kernel,
        name="store",
        out_shape=jax.ShapeDtypeStruct(held.shape, bf16),
        in_specs=[pl.BlockSpec(memory_space=pltpu.VMEM)],
        out_specs=pl.BlockSpec(memory_space=pltpu.HBM),
        scratch_shapes=[dma((fields,))],
        compiler_params=pltpu.CompilerParams(vmem_limit_bytes=8 * 1024 * 1024),
    )(held)


def solution(mesh):
    in_specs = (
        P(None, "lev", "horiz"),
        P("horiz"),
        P("horiz", None),
        P("horiz", None, None),
        P(None, ("horiz", "lev")),
        P(None, ("horiz", "lev")),
    )
    out_specs = P(None, None, ("horiz", "lev"))
    body = functools.partial(local, mesh.shape["lev"], mesh.shape["horiz"])
    return jax.shard_map(body, mesh=mesh, in_specs=in_specs, out_specs=out_specs, check_vma=False)
```

```python
import functools

import jax
import jax.numpy as jnp
from jax import lax
from jax.experimental import pallas as pl
from jax.experimental.pallas import tpu as pltpu
from jax.sharding import PartitionSpec as P

MESH = pl.DeviceIdType.MESH
HIGH = 256
LANES = 128


def round_up(value, step):
    return (value + step - 1) // step * step


def row_plan(fields, slab_levels):
    whole = slab_levels // 16 * 16
    rest = slab_levels - whole
    extra = round_up(fields * rest, 8)
    base = round_up(extra, 16)
    return whole, rest, extra, base, base + fields * whole


def field_groups(fields):
    first = max(1, fields // 5)
    second = (fields - first + 1) // 2
    cuts = [0, first, first + second, (first + second + fields) // 2, fields]
    return [(a, b) for a, b in zip(cuts[:-1], cuts[1:]) if b > a]


def rows_at(table, index):
    numbers = lax.GatherDimensionNumbers(
        offset_dims=(),
        collapsed_slice_dims=(0,),
        start_index_map=(0,),
        operand_batching_dims=(1,),
        start_indices_batching_dims=(1,),
    )
    return lax.gather(
        table, index[..., None], numbers, slice_sizes=(1, 1), mode=lax.GatherScatterMode.PROMISE_IN_BOUNDS
    )


def regrid_kernel(
    groups, levs, depth,
    inter_hbm, index_hbm, source_hbm, blocks_hbm, bracket_hbm, fraction_hbm, out_ref,
    inter_ref, index_ref, tile, spare, first_rows, other_rows, weights, request, wanted, chosen, arrived, total, slab, got,
    brackets, fractions, raw, table,
    inter_sem, index_sem, tile_sem, weight_sem, bracket_sem, fraction_sem,
    req_send, req_recv, val_send, val_recv, lev_send, lev_recv, all_above,
):
    fields, slab_levels, cells = tile.shape
    whole, rest, extra, base, rows = row_plan(fields, slab_levels)
    count = 2 * depth + 1
    wide = index_ref.shape[1]
    me = lax.axis_index("horiz")
    my_lev = lax.axis_index("lev")
    levels_out, columns = brackets.shape
    plan = field_groups(fields)
    chunks = [(base + a * whole, (b - a) * whole) for a, b in plan]
    parts = [[i] for i in range(len(chunks))]
    spans = list(chunks)
    if extra:
        parts[0].append(len(chunks))
        spans[0] = (0, base + chunks[0][1])
        chunks.append((0, extra))

    barrier = pltpu.get_barrier_semaphore()
    offsets = [o for o in range(-depth, depth + 1) if o != 0]
    for offset in offsets:
        pl.semaphore_signal(
            barrier, inc=1, device_id={"horiz": lax.rem(me + offset + groups, groups)}, device_id_type=MESH
        )
    has_below, has_above = my_lev > 0, my_lev < levs - 1

    def tell(semaphore, lev):
        pl.semaphore_signal(semaphore, inc=1, device_id={"lev": lev}, device_id_type=MESH)

    for hop in range(1, levs):
        pl.when(my_lev + hop < levs)(functools.partial(tell, barrier, my_lev + hop))
    greeted = len(offsets) + my_lev

    inter_copy = pltpu.make_async_copy(inter_hbm, inter_ref, inter_sem)
    inter_copy.start()
    index_copy = pltpu.make_async_copy(index_hbm, index_ref, index_sem)
    index_copy.start()
    tile_copy = pltpu.make_async_copy(source_hbm, tile, tile_sem)
    tile_copy.start()
    for part in range(levs):
        copy = pltpu.make_async_copy(
            blocks_hbm.at[:, :, pl.ds(part * columns, columns)], weights.at[:, part], weight_sem
        )
        copy.start()
    bracket_copy = pltpu.make_async_copy(bracket_hbm, brackets, bracket_sem)
    bracket_copy.start()
    fraction_copy = pltpu.make_async_copy(fraction_hbm, fractions, fraction_sem)
    fraction_copy.start()
    inter_copy.wait()
    index_copy.wait()
    slots = []
    for place in range(count):
        group = lax.rem(me + place - depth + groups, groups)
        cells_wanted = jnp.zeros((1, wide), jnp.int32)
        slot = jnp.int32(0)
        for k in range(count):
            hit = (inter_ref[k] == group).astype(jnp.int32)
            cells_wanted = cells_wanted + index_ref[k : k + 1, :] * hit
            slot = jnp.where(inter_ref[k] == group, jnp.int32(k), slot)
        slots.append(slot)
        if place == depth:
            wanted[place] = cells_wanted
        else:
            request[place] = cells_wanted

    def request_copy(place):
        return pltpu.make_async_remote_copy(
            src_ref=request.at[place],
            dst_ref=wanted.at[2 * depth - place],
            send_sem=req_send,
            recv_sem=req_recv.at[2 * depth - place],
            device_id={"horiz": lax.rem(me + place - depth + groups, groups)},
            device_id_type=MESH,
        )

    def value_copy(place, piece, sign):
        first, size = chunks[piece]
        return pltpu.make_async_remote_copy(
            src_ref=chosen.at[place, pl.ds(first, size)],
            dst_ref=arrived.at[2 * depth - place, pl.ds(first, size)],
            send_sem=val_send,
            recv_sem=val_recv.at[sign],
            device_id={"horiz": lax.rem(me + place - depth + groups, groups)},
            device_id_type=MESH,
        )

    def tally(ref, send_sem, recv_sem):
        return pltpu.make_async_remote_copy(
            src_ref=ref,
            dst_ref=ref,
            send_sem=send_sem,
            recv_sem=recv_sem,
            device_id={"lev": dest_of(0)},
            device_id_type=MESH,
        )

    weight_of = [sum(chunks[piece][1] for piece in part) for part in parts]
    sent_rows = sum(weight_of)

    upper = 2 * my_lev >= levs

    def dest_of(turn):
        return turn + (turn >= my_lev).astype(jnp.int32)

    def lev_copy(turn, number, piece):
        block = pl.ds(*chunks[piece])
        return pltpu.make_async_remote_copy(
            src_ref=slab.at[turn, block],
            dst_ref=got.at[my_lev, block],
            send_sem=lev_send,
            recv_sem=lev_recv.at[number],
            device_id={"lev": dest_of(turn)},
            device_id_type=MESH,
        )

    pl.semaphore_wait(barrier, greeted)
    pl.when((my_lev == levs - 1) & has_below)(lambda: tell(all_above, my_lev - 1))
    for reach in range(depth, 0, -1):
        request_copy(depth - reach).start()
        request_copy(depth + reach).start()

    tile_copy.wait()
    high_count = cells // HIGH
    head = spans[0][1]
    tail = rows - head
    if base:
        spare[...] = jnp.zeros(spare.shape, jnp.float32)
        for field in range(fields):
            if rest:
                spare[pl.ds(field * rest, rest), :] = tile[field, pl.ds(whole, rest), :].astype(jnp.float32)
    for chunk in range(high_count):
        lane = pl.ds(chunk * HIGH, HIGH)
        if base:
            first_rows[pl.ds(chunk * head, base), :] = spare[:, lane].astype(jnp.bfloat16)
        for field in range(fields):
            if field < plan[0][1]:
                spot = first_rows.at[pl.ds(chunk * head + base + field * whole, whole)]
            else:
                spot = other_rows.at[pl.ds(chunk * tail + base + field * whole - head, whole)]
            spot[...] = tile[field, pl.ds(0, whole), lane]

    ids = lax.broadcasted_iota(jnp.int32, (HIGH, 1), 0).astype(jnp.float32).astype(jnp.bfloat16)

    def select(place, held):
        cell = wanted[place]
        high = cell // HIGH
        low = (cell - high * HIGH).astype(jnp.float32).astype(jnp.bfloat16)
        picker = jnp.where(ids == low, jnp.bfloat16(1), jnp.bfloat16(0))
        found = jnp.dot(held[...], picker, preferred_element_type=jnp.float32)
        size = held.shape[0] // high_count
        values = jnp.zeros((size, wide), jnp.float32)
        for chunk in range(high_count):
            values = jnp.where(high == chunk, found[chunk * size : (chunk + 1) * size], values)
        return values.astype(jnp.bfloat16)

    first_span, other_span = pl.ds(0, head), pl.ds(head, tail)
    arrived[depth, first_span] = select(depth, first_rows)
    arrived[depth, other_span] = select(depth, other_rows)

    def hand_down():
        pl.semaphore_wait(all_above, 1)
        tell(all_above, my_lev - 1)

    between = has_below & has_above
    pl.when(between & upper)(hand_down)

    lean = 1 - 2 * (me % 2)

    def order_place(step):
        reach = depth - step // 2
        return depth + reach * (2 * (step % 2) - 1) * lean

    last = 2 * depth - 1

    def serve(step, carry):
        place = order_place(step)
        request_copy(2 * depth - place).wait_recv()
        chosen[place, first_span] = select(place, first_rows)
        for piece in parts[0]:
            value_copy(place, piece, 0).start()
        return carry

    lax.fori_loop(0, last, serve, 0)

    pl.when(between & jnp.logical_not(upper))(hand_down)

    def serve_rest(step, carry):
        place = order_place(step)
        chosen[place, other_span] = select(place, other_rows)
        for piece in parts[1]:
            value_copy(place, piece, 1).start()
        return carry

    lax.fori_loop(0, last, serve_rest, 0)
    for later in range(2, len(parts)):
        for step in range(last):
            for piece in parts[later]:
                value_copy(order_place(step), piece, later).start()
    near = order_place(last)
    request_copy(2 * depth - near).wait_recv()
    chosen[near, first_span] = select(near, first_rows)
    chosen[near, other_span] = select(near, other_rows)
    for piece in range(len(chunks)):
        value_copy(near, piece, len(parts)).start()

    pltpu.make_async_copy(weights, weights, weight_sem).wait()

    def slot_of(place):
        slot = slots[0]
        for k in range(1, count):
            slot = jnp.where(place == k, slots[k], slot)
        return slot

    values = arrived[depth]
    for part in range(levs):
        total[part] = jnp.dot(values, weights[slots[depth], part], preferred_element_type=jnp.float32)
    tally(arrived.at[0, pl.ds(0, sent_rows)], val_send, val_recv.at[len(parts)]).wait_recv()
    values = arrived[near]
    near_slot = slot_of(near)
    for part in range(levs):
        total[part] += jnp.dot(values, weights[near_slot, part], preferred_element_type=jnp.float32)

    def send_others(number):
        for turn in range(1, levs - 1):
            for piece in parts[number]:
                lev_copy(turn, number, piece).start()

    if levs > 1:
        pl.when(my_lev == 0)(lambda: pl.semaphore_wait(all_above, 1))
    far = [order_place(step) for step in range(last)]
    far_slots = [slot_of(place) for place in far]
    for number in range(len(parts)):
        tally(arrived.at[pl.ds(0, last), pl.ds(0, weight_of[number])], val_send, val_recv.at[number]).wait_recv()

        def column_sum(part, block, values):
            sums = total[part, block]
            for value, slot in zip(values, far_slots):
                sums += jnp.dot(value, weights[slot, part], preferred_element_type=jnp.float32)
            return sums.astype(jnp.bfloat16)

        block = pl.ds(*spans[number])
        values = [arrived[place, block] for place in far]
        slab[0, block] = column_sum(dest_of(0), block, values)
        for piece in parts[number]:
            lev_copy(0, number, piece).start()
        if number == len(parts) - 2:
            continue
        members = [number]
        if number == len(parts) - 1:
            pl.when(upper)(functools.partial(send_others, len(parts) - 3))
            members = [number - 1, number]
            block = pl.ds(spans[number - 1][0], spans[number - 1][1] + spans[number][1])
            values = [arrived[place, block] for place in far]
        for turn in range(1, levs - 1):
            slab[turn, block] = column_sum(dest_of(turn), block, values)
        got[my_lev, block] = column_sum(my_lev, block, values)
        for member in members:
            if member != len(parts) - 3:
                send_others(member)
            else:
                pl.when(jnp.logical_not(upper))(functools.partial(send_others, member))

    bracket_copy.wait()
    fraction_copy.wait()
    levels_in = levs * slab_levels
    step_rows = 16
    table[:, pl.ds(levels_in, table.shape[1] - levels_in), :] = jnp.zeros(
        (table.shape[0], table.shape[1] - levels_in, LANES), jnp.float32
    )

    def interpolate(first, end):
        held = list(range(first, end))

        def work(strip, carry):
            lane = pl.ds(pl.multiple_of(strip * LANES, LANES), LANES)
            for lev in range(levs):
                if rest:
                    raw[lev] = got[lev, pl.ds(0, base), lane].astype(jnp.float32)
                for place, field in enumerate(held):
                    table[place, pl.ds(lev * slab_levels, whole), :] = got[
                        lev, pl.ds(base + field * whole, whole), lane
                    ].astype(jnp.float32)
                    if rest:
                        table[place, pl.ds(lev * slab_levels + whole, rest), :] = raw[
                            lev, pl.ds(field * rest, rest), :
                        ]
            for start in range(0, levels_out, step_rows):
                size = min(step_rows, levels_out - start)
                bracket = brackets[start : start + size, lane]
                upper = fractions[start : start + size, lane]
                if size < step_rows:
                    bracket = jnp.concatenate([bracket, jnp.zeros((step_rows - size, LANES), jnp.int32)], axis=0)
                    upper = jnp.concatenate([upper, jnp.zeros((step_rows - size, LANES), jnp.float32)], axis=0)
                halves = [bracket[i : i + 8] for i in range(0, step_rows, 8)]
                high = [half >> 3 for half in halves]
                low = [half & 7 for half in halves]
                below = [[jnp.zeros((8, LANES), jnp.float32) for _ in halves] for _ in held]
                above = [[jnp.zeros((8, LANES), jnp.float32) for _ in halves] for _ in held]
                for group in range((levels_in - 2) // 8 + 1):
                    masks = [h == group for h in high]
                    for place in range(len(held)):
                        here = table[place, pl.ds(group * 8, 8), :]
                        over = table[place, pl.ds(group * 8 + 1, 8), :]
                        for i, mask in enumerate(masks):
                            below[place][i] = jnp.where(mask, rows_at(here, low[i]), below[place][i])
                            above[place][i] = jnp.where(mask, rows_at(over, low[i]), above[place][i])
                for place, field in enumerate(held):
                    mixed = (1.0 - upper) * jnp.concatenate(below[place], axis=0) + upper * jnp.concatenate(
                        above[place], axis=0
                    )
                    out_ref[field, start : start + size, lane] = mixed[:size].astype(jnp.bfloat16)
            return carry

        lax.fori_loop(0, columns // LANES, work, 0)

    for number, (first, end) in enumerate(plan):
        tally(got.at[pl.ds(0, levs - 1), pl.ds(0, weight_of[number])], lev_send, lev_recv.at[number]).wait_recv()
        interpolate(first, end)

    tally(slab.at[:, pl.ds(0, sent_rows)], lev_send, lev_recv.at[0]).wait_send()
    tally(chosen.at[pl.ds(0, 2 * depth), pl.ds(0, sent_rows)], val_send, val_recv.at[0]).wait_send()
    tally(request.at[pl.ds(0, 2 * depth)], req_send, req_recv.at[0]).wait_send()


def store_kernel(held_ref, out_hbm, sem):
    copies = [
        pltpu.make_async_copy(held_ref, out_hbm, sem)
    ]
    for copy in copies:
        copy.start()
    for copy in copies:
        copy.wait()


def local(levs, groups, source_state, intersection, index_map, blocks, bracket, fraction):
    fields, slab_levels, cells = source_state.shape
    count, wide, targets = blocks.shape
    depth = (count - 1) // 2
    whole, rest, extra, base, rows = row_plan(fields, slab_levels)
    columns = targets // levs
    levels_out = bracket.shape[0]
    plan = field_groups(fields)
    most = max(b - a for a, b in plan)
    head = base + plan[0][1] * whole
    bf16, f32, i32 = jnp.bfloat16, jnp.float32, jnp.int32
    dma = pltpu.SemaphoreType.DMA
    held = pl.pallas_call(
        functools.partial(regrid_kernel, groups, levs, depth),
        name="regrid",
        out_shape=pltpu.VMEM((fields, levels_out, columns), bf16),
        in_specs=[pl.BlockSpec(memory_space=pltpu.HBM)] * 6,
        out_specs=pl.BlockSpec(memory_space=pltpu.VMEM),
        scratch_shapes=[
            pltpu.SMEM((count,), i32),
            pltpu.VMEM((count, wide), i32),
            pltpu.VMEM((fields, slab_levels, cells), bf16),
            pltpu.VMEM((max(base, 8), cells), f32),
            pltpu.VMEM((cells // HIGH * head, HIGH), bf16),
            pltpu.VMEM((cells // HIGH * (rows - head), HIGH), bf16),
            pltpu.VMEM((count, levs, wide, columns), bf16),
            pltpu.VMEM((count, 1, wide), i32),
            pltpu.VMEM((count, 1, wide), i32),
            pltpu.VMEM((count, rows, wide), bf16),
            pltpu.VMEM((count, rows, wide), bf16),
            pltpu.VMEM((levs, rows, columns), f32),
            pltpu.VMEM((levs - 1, rows, columns), bf16),
            pltpu.VMEM((levs, rows, columns), bf16),
            pltpu.VMEM((levels_out, columns), i32),
            pltpu.VMEM((levels_out, columns), f32),
            pltpu.VMEM((levs, max(base, 8), LANES), f32),
            pltpu.VMEM((most, round_up(levs * slab_levels, 8) + 8, LANES), f32),
            dma,
            dma,
            dma,
            dma,
            dma,
            dma,
            dma,
            dma((count,)),
            dma,
            dma((len(plan) + 1,)),
            dma,
            dma((len(plan),)),
            pltpu.SemaphoreType.REGULAR,
        ],
        compiler_params=pltpu.CompilerParams(
            collective_id=0, has_side_effects=True, vmem_limit_bytes=56 * 1024 * 1024
        ),
        cost_estimate=pl.CostEstimate(
            flops=2 * rows * count * wide * (cells + targets),
            bytes_accessed=2 * blocks.size + 2 * source_state.size,
            transcendentals=0,
        ),
    )(intersection, index_map, source_state, blocks, bracket, fraction)
    return pl.pallas_call(
        store_kernel,
        name="store",
        out_shape=jax.ShapeDtypeStruct(held.shape, bf16),
        in_specs=[pl.BlockSpec(memory_space=pltpu.VMEM)],
        out_specs=pl.BlockSpec(memory_space=pltpu.HBM),
        scratch_shapes=[dma],
        compiler_params=pltpu.CompilerParams(vmem_limit_bytes=8 * 1024 * 1024),
    )(held)


def solution(mesh):
    in_specs = (
        P(None, "lev", "horiz"),
        P("horiz"),
        P("horiz", None),
        P("horiz", None, None),
        P(None, ("horiz", "lev")),
        P(None, ("horiz", "lev")),
    )
    out_specs = P(None, None, ("horiz", "lev"))
    body = functools.partial(local, mesh.shape["lev"], mesh.shape["horiz"])
    return jax.shard_map(body, mesh=mesh, in_specs=in_specs, out_specs=out_specs, check_vma=False)
```

```python
import functools

import jax
import jax.numpy as jnp
from jax import lax
from jax.experimental import pallas as pl
from jax.experimental.pallas import tpu as pltpu
from jax.sharding import PartitionSpec as P

MESH = pl.DeviceIdType.MESH
HIGH = 256
LANES = 128


def round_up(value, step):
    return (value + step - 1) // step * step


def row_plan(fields, slab_levels):
    whole = slab_levels // 16 * 16
    rest = slab_levels - whole
    extra = round_up(fields * rest, 8)
    base = round_up(extra, 16)
    return whole, rest, extra, base, base + fields * whole


def field_groups(fields):
    first = max(1, fields // 5)
    second = (fields - first + 1) // 2
    cuts = [0, first, first + second, (first + second + fields) // 2, fields]
    return [(a, b) for a, b in zip(cuts[:-1], cuts[1:]) if b > a]


def rows_at(table, index):
    numbers = lax.GatherDimensionNumbers(
        offset_dims=(),
        collapsed_slice_dims=(0,),
        start_index_map=(0,),
        operand_batching_dims=(1,),
        start_indices_batching_dims=(1,),
    )
    return lax.gather(
        table, index[..., None], numbers, slice_sizes=(1, 1), mode=lax.GatherScatterMode.PROMISE_IN_BOUNDS
    )


def regrid_kernel(
    groups, levs, depth,
    inter_hbm, index_hbm, source_hbm, blocks_hbm, bracket_hbm, fraction_hbm, out_ref,
    inter_ref, index_ref, tile, spare, first_rows, other_rows, weights, request, wanted, chosen, arrived, total, slab, got,
    brackets, fractions, raw, table,
    inter_sem, index_sem, tile_sem, weight_sem, bracket_sem, fraction_sem,
    req_send, req_recv, val_send, val_recv, lev_send, lev_recv, all_above,
):
    fields, slab_levels, cells = tile.shape
    whole, rest, extra, base, rows = row_plan(fields, slab_levels)
    count = 2 * depth + 1
    wide = index_ref.shape[1]
    me = lax.axis_index("horiz")
    my_lev = lax.axis_index("lev")
    levels_out, columns = brackets.shape
    plan = field_groups(fields)
    chunks = [(base + a * whole, (b - a) * whole) for a, b in plan]
    parts = [[i] for i in range(len(chunks))]
    spans = list(chunks)
    if extra:
        parts[0].append(len(chunks))
        spans[0] = (0, base + chunks[0][1])
        chunks.append((0, extra))

    barrier = pltpu.get_barrier_semaphore()
    offsets = [o for o in range(-depth, depth + 1) if o != 0]
    for offset in offsets:
        pl.semaphore_signal(
            barrier, inc=1, device_id={"horiz": lax.rem(me + offset + groups, groups)}, device_id_type=MESH
        )
    has_below, has_above = my_lev > 0, my_lev < levs - 1

    def tell(semaphore, lev):
        pl.semaphore_signal(semaphore, inc=1, device_id={"lev": lev}, device_id_type=MESH)

    for hop in range(1, levs):
        pl.when(my_lev + hop < levs)(functools.partial(tell, barrier, my_lev + hop))
    greeted = len(offsets) + my_lev

    inter_copy = pltpu.make_async_copy(inter_hbm, inter_ref, inter_sem)
    inter_copy.start()
    index_copy = pltpu.make_async_copy(index_hbm, index_ref, index_sem)
    index_copy.start()
    tile_copy = pltpu.make_async_copy(source_hbm, tile, tile_sem)
    tile_copy.start()
    for part in range(levs):
        copy = pltpu.make_async_copy(
            blocks_hbm.at[:, :, pl.ds(part * columns, columns)], weights.at[:, part], weight_sem
        )
        copy.start()
    bracket_copy = pltpu.make_async_copy(bracket_hbm, brackets, bracket_sem)
    bracket_copy.start()
    fraction_copy = pltpu.make_async_copy(fraction_hbm, fractions, fraction_sem)
    fraction_copy.start()
    inter_copy.wait()
    index_copy.wait()
    slots = []
    for place in range(count):
        group = lax.rem(me + place - depth + groups, groups)
        cells_wanted = jnp.zeros((1, wide), jnp.int32)
        slot = jnp.int32(0)
        for k in range(count):
            hit = (inter_ref[k] == group).astype(jnp.int32)
            cells_wanted = cells_wanted + index_ref[k : k + 1, :] * hit
            slot = jnp.where(inter_ref[k] == group, jnp.int32(k), slot)
        slots.append(slot)
        if place == depth:
            wanted[place] = cells_wanted
        else:
            request[place] = cells_wanted

    def request_copy(place):
        return pltpu.make_async_remote_copy(
            src_ref=request.at[place],
            dst_ref=wanted.at[2 * depth - place],
            send_sem=req_send,
            recv_sem=req_recv.at[2 * depth - place],
            device_id={"horiz": lax.rem(me + place - depth + groups, groups)},
            device_id_type=MESH,
        )

    def value_copy(place, piece, sign):
        first, size = chunks[piece]
        return pltpu.make_async_remote_copy(
            src_ref=chosen.at[place, pl.ds(first, size)],
            dst_ref=arrived.at[2 * depth - place, pl.ds(first, size)],
            send_sem=val_send,
            recv_sem=val_recv.at[sign],
            device_id={"horiz": lax.rem(me + place - depth + groups, groups)},
            device_id_type=MESH,
        )

    def tally(ref, send_sem, recv_sem):
        return pltpu.make_async_remote_copy(
            src_ref=ref,
            dst_ref=ref,
            send_sem=send_sem,
            recv_sem=recv_sem,
            device_id={"lev": dest_of(0)},
            device_id_type=MESH,
        )

    weight_of = [sum(chunks[piece][1] for piece in part) for part in parts]
    sent_rows = sum(weight_of)

    upper = 2 * my_lev >= levs

    def dest_of(turn):
        return turn + (turn >= my_lev).astype(jnp.int32)

    sides = [(0, columns // 2), (columns // 2, columns // 2)]

    def lev_copies(turn, number):
        spread = sides if number == len(parts) - 1 else [(0, columns)]
        return [
            lev_copy(turn, number + side, piece, pl.ds(*lane))
            for side, lane in enumerate(spread)
            for piece in parts[number]
        ]

    def lev_copy(turn, number, piece, lane):
        block = pl.ds(*chunks[piece])
        return pltpu.make_async_remote_copy(
            src_ref=slab.at[turn, block, lane],
            dst_ref=got.at[my_lev, block, lane],
            send_sem=lev_send,
            recv_sem=lev_recv.at[number],
            device_id={"lev": dest_of(turn)},
            device_id_type=MESH,
        )

    pl.semaphore_wait(barrier, greeted)
    pl.when((my_lev == levs - 1) & has_below)(lambda: tell(all_above, my_lev - 1))
    for reach in range(depth, 0, -1):
        request_copy(depth - reach).start()
        request_copy(depth + reach).start()

    tile_copy.wait()
    high_count = cells // HIGH
    head = spans[0][1]
    tail = rows - head
    if base:
        spare[...] = jnp.zeros(spare.shape, jnp.float32)
        for field in range(fields):
            if rest:
                spare[pl.ds(field * rest, rest), :] = tile[field, pl.ds(whole, rest), :].astype(jnp.float32)
    for chunk in range(high_count):
        lane = pl.ds(chunk * HIGH, HIGH)
        if base:
            first_rows[pl.ds(chunk * head, base), :] = spare[:, lane].astype(jnp.bfloat16)
        for field in range(fields):
            if field < plan[0][1]:
                spot = first_rows.at[pl.ds(chunk * head + base + field * whole, whole)]
            else:
                spot = other_rows.at[pl.ds(chunk * tail + base + field * whole - head, whole)]
            spot[...] = tile[field, pl.ds(0, whole), lane]

    ids = lax.broadcasted_iota(jnp.int32, (HIGH, 1), 0).astype(jnp.float32).astype(jnp.bfloat16)

    def select(place, held):
        cell = wanted[place]
        high = cell // HIGH
        low = (cell - high * HIGH).astype(jnp.float32).astype(jnp.bfloat16)
        picker = jnp.where(ids == low, jnp.bfloat16(1), jnp.bfloat16(0))
        found = jnp.dot(held[...], picker, preferred_element_type=jnp.float32)
        size = held.shape[0] // high_count
        values = jnp.zeros((size, wide), jnp.float32)
        for chunk in range(high_count):
            values = jnp.where(high == chunk, found[chunk * size : (chunk + 1) * size], values)
        return values.astype(jnp.bfloat16)

    first_span, other_span = pl.ds(0, head), pl.ds(head, tail)
    arrived[depth, first_span] = select(depth, first_rows)
    arrived[depth, other_span] = select(depth, other_rows)

    def hand_down():
        pl.semaphore_wait(all_above, 1)
        tell(all_above, my_lev - 1)

    between = has_below & has_above
    pl.when(between & upper)(hand_down)

    lean = 1 - 2 * (me % 2)

    def order_place(step):
        reach = depth - step // 2
        return depth + reach * (2 * (step % 2) - 1) * lean

    last = 2 * depth - 1

    near = order_place(last)
    request_copy(2 * depth - near).wait_recv()
    chosen[near, first_span] = select(near, first_rows)
    chosen[near, other_span] = select(near, other_rows)
    for piece in range(len(chunks)):
        value_copy(near, piece, len(parts)).start()

    def serve(step, carry):
        place = order_place(step)
        request_copy(2 * depth - place).wait_recv()
        chosen[place, first_span] = select(place, first_rows)
        for piece in parts[0]:
            value_copy(place, piece, 0).start()
        return carry

    lax.fori_loop(0, last, serve, 0)

    pl.when(between & jnp.logical_not(upper))(hand_down)

    def serve_rest(step, carry):
        place = order_place(step)
        chosen[place, other_span] = select(place, other_rows)
        for piece in parts[1]:
            value_copy(place, piece, 1).start()
        return carry

    lax.fori_loop(0, last, serve_rest, 0)
    for later in range(2, len(parts)):
        for step in range(last):
            for piece in parts[later]:
                value_copy(order_place(step), piece, later).start()
    pltpu.make_async_copy(weights, weights, weight_sem).wait()

    def slot_of(place):
        slot = slots[0]
        for k in range(1, count):
            slot = jnp.where(place == k, slots[k], slot)
        return slot

    tally(arrived.at[0, pl.ds(0, sent_rows)], val_send, val_recv.at[len(parts)]).wait_recv()
    beside = [(arrived[depth], slots[depth]), (arrived[near], slot_of(near))]
    for part in range(levs):
        total[part] = sum(
            jnp.dot(value, weights[slot, part], preferred_element_type=jnp.float32) for value, slot in beside
        )

    def send_others(number):
        for turn in range(1, levs - 1):
            for copy in lev_copies(turn, number):
                copy.start()

    if levs > 1:
        pl.when(my_lev == 0)(lambda: pl.semaphore_wait(all_above, 1))
    far = [order_place(step) for step in range(last)]
    far_slots = [slot_of(place) for place in far]
    for number in range(len(parts)):
        tally(arrived.at[pl.ds(0, last), pl.ds(0, weight_of[number])], val_send, val_recv.at[number]).wait_recv()

        def column_sum(part, block, values, lane=pl.ds(0, columns)):
            sums = total[part, block, lane]
            for value, slot in zip(values, far_slots):
                sums += jnp.dot(value, weights[slot, part, :, lane], preferred_element_type=jnp.float32)
            return sums.astype(jnp.bfloat16)

        block = pl.ds(*spans[number])
        values = [arrived[place, block] for place in far]
        copies = lev_copies(0, number)
        if number == len(parts) - 1:
            for side, copy in zip(sides, copies):
                lane = pl.ds(*side)
                slab[0, block, lane] = column_sum(dest_of(0), block, values, lane)
                copy.start()
        else:
            slab[0, block] = column_sum(dest_of(0), block, values)
            for copy in copies:
                copy.start()
        if number == len(parts) - 2:
            continue
        members = [number]
        if number == len(parts) - 1:
            pl.when(upper)(functools.partial(send_others, len(parts) - 3))
            members = [number - 1, number]
            block = pl.ds(spans[number - 1][0], spans[number - 1][1] + spans[number][1])
            values = [arrived[place, block] for place in far]
        for turn in range(1, levs - 1):
            slab[turn, block] = column_sum(dest_of(turn), block, values)
        got[my_lev, block] = column_sum(my_lev, block, values)
        for member in members:
            if member != len(parts) - 3:
                send_others(member)
            else:
                pl.when(jnp.logical_not(upper))(functools.partial(send_others, member))

    bracket_copy.wait()
    fraction_copy.wait()
    levels_in = levs * slab_levels
    step_rows = 16
    table[:, pl.ds(levels_in, table.shape[1] - levels_in), :] = jnp.zeros(
        (table.shape[0], table.shape[1] - levels_in, LANES), jnp.float32
    )

    def interpolate(first, end, low_strip, high_strip):
        held = list(range(first, end))

        def work(strip, carry):
            lane = pl.ds(pl.multiple_of(strip * LANES, LANES), LANES)
            for lev in range(levs):
                if rest:
                    raw[lev] = got[lev, pl.ds(0, base), lane].astype(jnp.float32)
                for place, field in enumerate(held):
                    table[place, pl.ds(lev * slab_levels, whole), :] = got[
                        lev, pl.ds(base + field * whole, whole), lane
                    ].astype(jnp.float32)
                    if rest:
                        table[place, pl.ds(lev * slab_levels + whole, rest), :] = raw[
                            lev, pl.ds(field * rest, rest), :
                        ]
            for start in range(0, levels_out, step_rows):
                size = min(step_rows, levels_out - start)
                bracket = brackets[start : start + size, lane]
                upper = fractions[start : start + size, lane]
                if size < step_rows:
                    bracket = jnp.concatenate([bracket, jnp.zeros((step_rows - size, LANES), jnp.int32)], axis=0)
                    upper = jnp.concatenate([upper, jnp.zeros((step_rows - size, LANES), jnp.float32)], axis=0)
                halves = [bracket[i : i + 8] for i in range(0, step_rows, 8)]
                high = [half >> 3 for half in halves]
                low = [half & 7 for half in halves]
                counts = (levels_in - 2) // 8 + 1
                bits = max(1, (counts - 1).bit_length())
                turns = [[(h & (1 << bit)) != 0 for bit in range(bits)] for h in high]

                def choose(place, first, size, i):
                    if size == 1:
                        here = table[place, pl.ds(first * 8, 8), :]
                        over = table[place, pl.ds(first * 8 + 1, 8), :]
                        return rows_at(here, low[i]), rows_at(over, low[i])
                    half = size // 2
                    left = choose(place, first, half, i)
                    if first + half >= counts:
                        return left
                    right = choose(place, first + half, half, i)
                    mask = turns[i][half.bit_length() - 1]
                    return tuple(jnp.where(mask, b, a) for a, b in zip(left, right))

                below = [[None] * len(halves) for _ in held]
                above = [[None] * len(halves) for _ in held]
                for place in range(len(held)):
                    for i in range(len(halves)):
                        below[place][i], above[place][i] = choose(place, 0, 1 << bits, i)
                for place, field in enumerate(held):
                    mixed = (1.0 - upper) * jnp.concatenate(below[place], axis=0) + upper * jnp.concatenate(
                        above[place], axis=0
                    )
                    out_ref[field, start : start + size, lane] = mixed[:size].astype(jnp.bfloat16)
            return carry

        lax.fori_loop(low_strip, high_strip, work, 0)

    for number, (first, end) in enumerate(plan):
        for side, (left, width) in enumerate(sides if number == len(parts) - 1 else [(0, columns)]):
            landed = got.at[pl.ds(0, levs - 1), pl.ds(0, weight_of[number]), pl.ds(0, width)]
            tally(landed, lev_send, lev_recv.at[number + side]).wait_recv()
            interpolate(first, end, left // LANES, (left + width) // LANES)

    tally(slab.at[:, pl.ds(0, sent_rows)], lev_send, lev_recv.at[0]).wait_send()
    tally(chosen.at[pl.ds(0, 2 * depth), pl.ds(0, sent_rows)], val_send, val_recv.at[0]).wait_send()
    tally(request.at[pl.ds(0, 2 * depth)], req_send, req_recv.at[0]).wait_send()


def store_kernel(held_ref, out_hbm, sem):
    copies = [
        pltpu.make_async_copy(held_ref, out_hbm, sem)
    ]
    for copy in copies:
        copy.start()
    for copy in copies:
        copy.wait()


def local(levs, groups, source_state, intersection, index_map, blocks, bracket, fraction):
    fields, slab_levels, cells = source_state.shape
    count, wide, targets = blocks.shape
    depth = (count - 1) // 2
    whole, rest, extra, base, rows = row_plan(fields, slab_levels)
    columns = targets // levs
    levels_out = bracket.shape[0]
    plan = field_groups(fields)
    most = max(b - a for a, b in plan)
    head = base + plan[0][1] * whole
    bf16, f32, i32 = jnp.bfloat16, jnp.float32, jnp.int32
    dma = pltpu.SemaphoreType.DMA
    held = pl.pallas_call(
        functools.partial(regrid_kernel, groups, levs, depth),
        name="regrid",
        out_shape=pltpu.VMEM((fields, levels_out, columns), bf16),
        in_specs=[pl.BlockSpec(memory_space=pltpu.HBM)] * 6,
        out_specs=pl.BlockSpec(memory_space=pltpu.VMEM),
        scratch_shapes=[
            pltpu.SMEM((count,), i32),
            pltpu.VMEM((count, wide), i32),
            pltpu.VMEM((fields, slab_levels, cells), bf16),
            pltpu.VMEM((max(base, 8), cells), f32),
            pltpu.VMEM((cells // HIGH * head, HIGH), bf16),
            pltpu.VMEM((cells // HIGH * (rows - head), HIGH), bf16),
            pltpu.VMEM((count, levs, wide, columns), bf16),
            pltpu.VMEM((count, 1, wide), i32),
            pltpu.VMEM((count, 1, wide), i32),
            pltpu.VMEM((count, rows, wide), bf16),
            pltpu.VMEM((count, rows, wide), bf16),
            pltpu.VMEM((levs, rows, columns), f32),
            pltpu.VMEM((levs - 1, rows, columns), bf16),
            pltpu.VMEM((levs, rows, columns), bf16),
            pltpu.VMEM((levels_out, columns), i32),
            pltpu.VMEM((levels_out, columns), f32),
            pltpu.VMEM((levs, max(base, 8), LANES), f32),
            pltpu.VMEM((most, round_up(levs * slab_levels, 8) + 8, LANES), f32),
            dma,
            dma,
            dma,
            dma,
            dma,
            dma,
            dma,
            dma((count,)),
            dma,
            dma((len(plan) + 1,)),
            dma,
            dma((len(plan) + 1,)),
            pltpu.SemaphoreType.REGULAR,
        ],
        compiler_params=pltpu.CompilerParams(
            collective_id=0, has_side_effects=True, vmem_limit_bytes=56 * 1024 * 1024
        ),
        cost_estimate=pl.CostEstimate(
            flops=2 * rows * count * wide * (cells + targets),
            bytes_accessed=2 * blocks.size + 2 * source_state.size,
            transcendentals=0,
        ),
    )(intersection, index_map, source_state, blocks, bracket, fraction)
    return pl.pallas_call(
        store_kernel,
        name="store",
        out_shape=jax.ShapeDtypeStruct(held.shape, bf16),
        in_specs=[pl.BlockSpec(memory_space=pltpu.VMEM)],
        out_specs=pl.BlockSpec(memory_space=pltpu.HBM),
        scratch_shapes=[dma],
        compiler_params=pltpu.CompilerParams(vmem_limit_bytes=8 * 1024 * 1024),
    )(held)


def solution(mesh):
    in_specs = (
        P(None, "lev", "horiz"),
        P("horiz"),
        P("horiz", None),
        P("horiz", None, None),
        P(None, ("horiz", "lev")),
        P(None, ("horiz", "lev")),
    )
    out_specs = P(None, None, ("horiz", "lev"))
    body = functools.partial(local, mesh.shape["lev"], mesh.shape["horiz"])
    return jax.shard_map(body, mesh=mesh, in_specs=in_specs, out_specs=out_specs, check_vma=False)
```

```python
import functools

import jax
import jax.numpy as jnp
from jax import lax
from jax.experimental import pallas as pl
from jax.experimental.pallas import tpu as pltpu
from jax.sharding import PartitionSpec as P

MESH = pl.DeviceIdType.MESH
HIGH = 256
LANES = 128


def round_up(value, step):
    return (value + step - 1) // step * step


def row_plan(fields, slab_levels):
    whole = slab_levels // 16 * 16
    rest = slab_levels - whole
    extra = round_up(fields * rest, 8)
    base = round_up(extra, 16)
    return whole, rest, extra, base, base + fields * whole


def field_groups(fields):
    first = max(1, fields // 5)
    second = (fields - first + 1) // 2
    cuts = [0, first, first + second, (first + second + fields) // 2, fields]
    return [(a, b) for a, b in zip(cuts[:-1], cuts[1:]) if b > a]


def rows_at(table, index):
    numbers = lax.GatherDimensionNumbers(
        offset_dims=(),
        collapsed_slice_dims=(0,),
        start_index_map=(0,),
        operand_batching_dims=(1,),
        start_indices_batching_dims=(1,),
    )
    return lax.gather(
        table, index[..., None], numbers, slice_sizes=(1, 1), mode=lax.GatherScatterMode.PROMISE_IN_BOUNDS
    )


def regrid_kernel(
    groups, levs, depth,
    inter_hbm, index_hbm, source_hbm, blocks_hbm, bracket_hbm, fraction_hbm, out_ref,
    inter_ref, index_ref, tile, spare, first_rows, other_rows, weights, request, wanted, chosen, arrived, total, slab, got,
    brackets, fractions, raw, table,
    inter_sem, index_sem, tile_sem, weight_sem, bracket_sem, fraction_sem,
    req_send, req_recv, val_send, val_recv, lev_send, lev_recv, all_above,
):
    fields, slab_levels, cells = tile.shape
    whole, rest, extra, base, rows = row_plan(fields, slab_levels)
    count = 2 * depth + 1
    wide = index_ref.shape[1]
    me = lax.axis_index("horiz")
    my_lev = lax.axis_index("lev")
    levels_out, columns = brackets.shape
    plan = field_groups(fields)
    chunks = [(base + a * whole, (b - a) * whole) for a, b in plan]
    parts = [[i] for i in range(len(chunks))]
    spans = list(chunks)
    if extra:
        parts[0].append(len(chunks))
        spans[0] = (0, base + chunks[0][1])
        chunks.append((0, extra))

    barrier = pltpu.get_barrier_semaphore()
    offsets = [o for o in range(-depth, depth + 1) if o != 0]
    for offset in offsets:
        pl.semaphore_signal(
            barrier, inc=1, device_id={"horiz": lax.rem(me + offset + groups, groups)}, device_id_type=MESH
        )
    has_below, has_above = my_lev > 0, my_lev < levs - 1

    def tell(semaphore, lev):
        pl.semaphore_signal(semaphore, inc=1, device_id={"lev": lev}, device_id_type=MESH)

    for hop in range(1, levs):
        pl.when(my_lev + hop < levs)(functools.partial(tell, barrier, my_lev + hop))
    greeted = len(offsets) + my_lev

    inter_copy = pltpu.make_async_copy(inter_hbm, inter_ref, inter_sem)
    inter_copy.start()
    index_copy = pltpu.make_async_copy(index_hbm, index_ref, index_sem)
    index_copy.start()
    tile_copy = pltpu.make_async_copy(source_hbm, tile, tile_sem)
    tile_copy.start()
    for part in range(levs):
        copy = pltpu.make_async_copy(
            blocks_hbm.at[:, :, pl.ds(part * columns, columns)], weights.at[:, part], weight_sem
        )
        copy.start()
    bracket_copy = pltpu.make_async_copy(bracket_hbm, brackets, bracket_sem)
    bracket_copy.start()
    fraction_copy = pltpu.make_async_copy(fraction_hbm, fractions, fraction_sem)
    fraction_copy.start()
    inter_copy.wait()
    index_copy.wait()
    slots = []
    for place in range(count):
        group = lax.rem(me + place - depth + groups, groups)
        cells_wanted = jnp.zeros((1, wide), jnp.int32)
        slot = jnp.int32(0)
        for k in range(count):
            hit = (inter_ref[k] == group).astype(jnp.int32)
            cells_wanted = cells_wanted + index_ref[k : k + 1, :] * hit
            slot = jnp.where(inter_ref[k] == group, jnp.int32(k), slot)
        slots.append(slot)
        if place == depth:
            wanted[place] = cells_wanted
        else:
            request[place] = cells_wanted

    def request_copy(place):
        return pltpu.make_async_remote_copy(
            src_ref=request.at[place],
            dst_ref=wanted.at[2 * depth - place],
            send_sem=req_send,
            recv_sem=req_recv.at[2 * depth - place],
            device_id={"horiz": lax.rem(me + place - depth + groups, groups)},
            device_id_type=MESH,
        )

    def value_copy(place, piece, sign):
        first, size = chunks[piece]
        return pltpu.make_async_remote_copy(
            src_ref=chosen.at[place, pl.ds(first, size)],
            dst_ref=arrived.at[2 * depth - place, pl.ds(first, size)],
            send_sem=val_send,
            recv_sem=val_recv.at[sign],
            device_id={"horiz": lax.rem(me + place - depth + groups, groups)},
            device_id_type=MESH,
        )

    def tally(ref, send_sem, recv_sem):
        return pltpu.make_async_remote_copy(
            src_ref=ref,
            dst_ref=ref,
            send_sem=send_sem,
            recv_sem=recv_sem,
            device_id={"lev": dest_of(0)},
            device_id_type=MESH,
        )

    weight_of = [sum(chunks[piece][1] for piece in part) for part in parts]
    sent_rows = sum(weight_of)

    upper = 2 * my_lev >= levs

    def dest_of(turn):
        return turn + (turn >= my_lev).astype(jnp.int32)

    sides = [(0, columns // 2), (columns // 2, columns // 2)]

    def lev_copies(turn, number):
        spread = sides if number == len(parts) - 1 else [(0, columns)]
        return [
            lev_copy(turn, number + side, piece, pl.ds(*lane))
            for side, lane in enumerate(spread)
            for piece in parts[number]
        ]

    def lev_copy(turn, number, piece, lane):
        block = pl.ds(*chunks[piece])
        return pltpu.make_async_remote_copy(
            src_ref=slab.at[turn, block, lane],
            dst_ref=got.at[my_lev, block, lane],
            send_sem=lev_send,
            recv_sem=lev_recv.at[number],
            device_id={"lev": dest_of(turn)},
            device_id_type=MESH,
        )

    pl.semaphore_wait(barrier, greeted)
    pl.when((my_lev == levs - 1) & has_below)(lambda: tell(all_above, my_lev - 1))
    for reach in range(depth, 0, -1):
        request_copy(depth - reach).start()
        request_copy(depth + reach).start()

    tile_copy.wait()
    high_count = cells // HIGH
    head = spans[0][1]
    tail = rows - head
    if base:
        spare[...] = jnp.zeros(spare.shape, jnp.float32)
        for field in range(fields):
            if rest:
                spare[pl.ds(field * rest, rest), :] = tile[field, pl.ds(whole, rest), :].astype(jnp.float32)
    for chunk in range(high_count):
        lane = pl.ds(chunk * HIGH, HIGH)
        if base:
            first_rows[pl.ds(chunk * head, base), :] = spare[:, lane].astype(jnp.bfloat16)
        for field in range(fields):
            if field < plan[0][1]:
                spot = first_rows.at[pl.ds(chunk * head + base + field * whole, whole)]
            else:
                spot = other_rows.at[pl.ds(chunk * tail + base + field * whole - head, whole)]
            spot[...] = tile[field, pl.ds(0, whole), lane]

    ids = lax.broadcasted_iota(jnp.int32, (HIGH, 1), 0).astype(jnp.float32).astype(jnp.bfloat16)

    def select(place, held):
        cell = wanted[place]
        high = cell // HIGH
        low = (cell - high * HIGH).astype(jnp.float32).astype(jnp.bfloat16)
        picker = jnp.where(ids == low, jnp.bfloat16(1), jnp.bfloat16(0))
        found = jnp.dot(held[...], picker, preferred_element_type=jnp.float32)
        size = held.shape[0] // high_count
        values = jnp.zeros((size, wide), jnp.float32)
        for chunk in range(high_count):
            values = jnp.where(high == chunk, found[chunk * size : (chunk + 1) * size], values)
        return values.astype(jnp.bfloat16)

    first_span, other_span = pl.ds(0, head), pl.ds(head, tail)
    arrived[depth, first_span] = select(depth, first_rows)
    arrived[depth, other_span] = select(depth, other_rows)

    def hand_down():
        pl.semaphore_wait(all_above, 1)
        tell(all_above, my_lev - 1)

    between = has_below & has_above
    pl.when(between & upper)(hand_down)

    lean = 1 - 2 * (me % 2)

    def order_place(step):
        reach = depth - step // 2
        return depth + reach * (2 * (step % 2) - 1) * lean

    last = 2 * depth - 1

    def serve(step, carry):
        place = order_place(step)
        request_copy(2 * depth - place).wait_recv()
        chosen[place, first_span] = select(place, first_rows)
        for piece in parts[0]:
            value_copy(place, piece, 0).start()
        return carry

    lax.fori_loop(0, last, serve, 0)
    near = order_place(last)
    request_copy(2 * depth - near).wait_recv()
    chosen[near, first_span] = select(near, first_rows)
    for piece in parts[0]:
        value_copy(near, piece, len(parts)).start()

    pl.when(between & jnp.logical_not(upper))(hand_down)

    def serve_rest(step, carry):
        place = order_place(step)
        chosen[place, other_span] = select(place, other_rows)
        for piece in parts[1]:
            value_copy(place, piece, 1).start()
        return carry

    lax.fori_loop(0, last, serve_rest, 0)
    for later in range(2, len(parts)):
        for step in range(last):
            for piece in parts[later]:
                value_copy(order_place(step), piece, later).start()
    chosen[near, other_span] = select(near, other_rows)
    for part in parts[1:]:
        for piece in part:
            value_copy(near, piece, len(parts) + 1).start()

    pltpu.make_async_copy(weights, weights, weight_sem).wait()

    def slot_of(place):
        slot = slots[0]
        for k in range(1, count):
            slot = jnp.where(place == k, slots[k], slot)
        return slot

    values = arrived[depth]
    for part in range(levs):
        total[part] = jnp.dot(values, weights[slots[depth], part], preferred_element_type=jnp.float32)
    near_slot = slot_of(near)

    def add_near(span, arrivals, sign):
        tally(arrived.at[0, pl.ds(0, arrivals)], val_send, val_recv.at[sign]).wait_recv()
        near_values = arrived[near, span]
        for part in range(levs):
            total[part, span] += jnp.dot(near_values, weights[near_slot, part], preferred_element_type=jnp.float32)

    add_near(first_span, weight_of[0], len(parts))

    def send_others(number):
        for turn in range(1, levs - 1):
            for copy in lev_copies(turn, number):
                copy.start()

    if levs > 1:
        pl.when(my_lev == 0)(lambda: pl.semaphore_wait(all_above, 1))
    far = [order_place(step) for step in range(last)]
    far_slots = [slot_of(place) for place in far]
    for number in range(len(parts)):
        tally(arrived.at[pl.ds(0, last), pl.ds(0, weight_of[number])], val_send, val_recv.at[number]).wait_recv()

        def column_sum(part, block, values, lane=pl.ds(0, columns)):
            sums = total[part, block, lane]
            for value, slot in zip(values, far_slots):
                sums += jnp.dot(value, weights[slot, part, :, lane], preferred_element_type=jnp.float32)
            return sums.astype(jnp.bfloat16)

        block = pl.ds(*spans[number])
        values = [arrived[place, block] for place in far]
        copies = lev_copies(0, number)
        if number == len(parts) - 1:
            for side, copy in zip(sides, copies):
                lane = pl.ds(*side)
                slab[0, block, lane] = column_sum(dest_of(0), block, values, lane)
                copy.start()
        else:
            slab[0, block] = column_sum(dest_of(0), block, values)
            for copy in copies:
                copy.start()
        if number == len(parts) - 2:
            continue
        members = [number]
        if number == len(parts) - 1:
            pl.when(upper)(functools.partial(send_others, len(parts) - 3))
            members = [number - 1, number]
            block = pl.ds(spans[number - 1][0], spans[number - 1][1] + spans[number][1])
            values = [arrived[place, block] for place in far]
        for turn in range(1, levs - 1):
            slab[turn, block] = column_sum(dest_of(turn), block, values)
        got[my_lev, block] = column_sum(my_lev, block, values)
        for member in members:
            if member != len(parts) - 3:
                send_others(member)
            else:
                pl.when(jnp.logical_not(upper))(functools.partial(send_others, member))
        if number == 0:
            add_near(other_span, sent_rows - weight_of[0], len(parts) + 1)

    bracket_copy.wait()
    fraction_copy.wait()
    levels_in = levs * slab_levels
    step_rows = 16
    table[:, pl.ds(levels_in, table.shape[1] - levels_in), :] = jnp.zeros(
        (table.shape[0], table.shape[1] - levels_in, LANES), jnp.float32
    )

    def interpolate(first, end, low_strip, high_strip):
        held = list(range(first, end))

        def work(strip, carry):
            lane = pl.ds(pl.multiple_of(strip * LANES, LANES), LANES)
            for lev in range(levs):
                if rest:
                    raw[lev] = got[lev, pl.ds(0, base), lane].astype(jnp.float32)
                for place, field in enumerate(held):
                    table[place, pl.ds(lev * slab_levels, whole), :] = got[
                        lev, pl.ds(base + field * whole, whole), lane
                    ].astype(jnp.float32)
                    if rest:
                        table[place, pl.ds(lev * slab_levels + whole, rest), :] = raw[
                            lev, pl.ds(field * rest, rest), :
                        ]
            for start in range(0, levels_out, step_rows):
                size = min(step_rows, levels_out - start)
                bracket = brackets[start : start + size, lane]
                upper = fractions[start : start + size, lane]
                if size < step_rows:
                    bracket = jnp.concatenate([bracket, jnp.zeros((step_rows - size, LANES), jnp.int32)], axis=0)
                    upper = jnp.concatenate([upper, jnp.zeros((step_rows - size, LANES), jnp.float32)], axis=0)
                halves = [bracket[i : i + 8] for i in range(0, step_rows, 8)]
                high = [half >> 3 for half in halves]
                low = [half & 7 for half in halves]
                counts = (levels_in - 2) // 8 + 1
                bits = max(1, (counts - 1).bit_length())
                turns = [[(h & (1 << bit)) != 0 for bit in range(bits)] for h in high]

                def choose(place, first, size, i):
                    if size == 1:
                        here = table[place, pl.ds(first * 8, 8), :]
                        over = table[place, pl.ds(first * 8 + 1, 8), :]
                        return rows_at(here, low[i]), rows_at(over, low[i])
                    half = size // 2
                    left = choose(place, first, half, i)
                    if first + half >= counts:
                        return left
                    right = choose(place, first + half, half, i)
                    mask = turns[i][half.bit_length() - 1]
                    return tuple(jnp.where(mask, b, a) for a, b in zip(left, right))

                below = [[None] * len(halves) for _ in held]
                above = [[None] * len(halves) for _ in held]
                for place in range(len(held)):
                    for i in range(len(halves)):
                        below[place][i], above[place][i] = choose(place, 0, 1 << bits, i)
                for place, field in enumerate(held):
                    mixed = (1.0 - upper) * jnp.concatenate(below[place], axis=0) + upper * jnp.concatenate(
                        above[place], axis=0
                    )
                    out_ref[field, start : start + size, lane] = mixed[:size].astype(jnp.bfloat16)
            return carry

        lax.fori_loop(low_strip, high_strip, work, 0)

    for number, (first, end) in enumerate(plan):
        for side, (left, width) in enumerate(sides if number == len(parts) - 1 else [(0, columns)]):
            landed = got.at[pl.ds(0, levs - 1), pl.ds(0, weight_of[number]), pl.ds(0, width)]
            tally(landed, lev_send, lev_recv.at[number + side]).wait_recv()
            interpolate(first, end, left // LANES, (left + width) // LANES)

    tally(slab.at[:, pl.ds(0, sent_rows)], lev_send, lev_recv.at[0]).wait_send()
    tally(chosen.at[pl.ds(0, 2 * depth), pl.ds(0, sent_rows)], val_send, val_recv.at[0]).wait_send()
    tally(request.at[pl.ds(0, 2 * depth)], req_send, req_recv.at[0]).wait_send()


def store_kernel(held_ref, out_hbm, sem):
    copies = [
        pltpu.make_async_copy(held_ref, out_hbm, sem)
    ]
    for copy in copies:
        copy.start()
    for copy in copies:
        copy.wait()


def local(levs, groups, source_state, intersection, index_map, blocks, bracket, fraction):
    fields, slab_levels, cells = source_state.shape
    count, wide, targets = blocks.shape
    depth = (count - 1) // 2
    whole, rest, extra, base, rows = row_plan(fields, slab_levels)
    columns = targets // levs
    levels_out = bracket.shape[0]
    plan = field_groups(fields)
    most = max(b - a for a, b in plan)
    head = base + plan[0][1] * whole
    bf16, f32, i32 = jnp.bfloat16, jnp.float32, jnp.int32
    dma = pltpu.SemaphoreType.DMA
    held = pl.pallas_call(
        functools.partial(regrid_kernel, groups, levs, depth),
        name="regrid",
        out_shape=pltpu.VMEM((fields, levels_out, columns), bf16),
        in_specs=[pl.BlockSpec(memory_space=pltpu.HBM)] * 6,
        out_specs=pl.BlockSpec(memory_space=pltpu.VMEM),
        scratch_shapes=[
            pltpu.SMEM((count,), i32),
            pltpu.VMEM((count, wide), i32),
            pltpu.VMEM((fields, slab_levels, cells), bf16),
            pltpu.VMEM((max(base, 8), cells), f32),
            pltpu.VMEM((cells // HIGH * head, HIGH), bf16),
            pltpu.VMEM((cells // HIGH * (rows - head), HIGH), bf16),
            pltpu.VMEM((count, levs, wide, columns), bf16),
            pltpu.VMEM((count, 1, wide), i32),
            pltpu.VMEM((count, 1, wide), i32),
            pltpu.VMEM((count, rows, wide), bf16),
            pltpu.VMEM((count, rows, wide), bf16),
            pltpu.VMEM((levs, rows, columns), f32),
            pltpu.VMEM((levs - 1, rows, columns), bf16),
            pltpu.VMEM((levs, rows, columns), bf16),
            pltpu.VMEM((levels_out, columns), i32),
            pltpu.VMEM((levels_out, columns), f32),
            pltpu.VMEM((levs, max(base, 8), LANES), f32),
            pltpu.VMEM((most, round_up(levs * slab_levels, 8) + 8, LANES), f32),
            dma,
            dma,
            dma,
            dma,
            dma,
            dma,
            dma,
            dma((count,)),
            dma,
            dma((len(plan) + 2,)),
            dma,
            dma((len(plan) + 1,)),
            pltpu.SemaphoreType.REGULAR,
        ],
        compiler_params=pltpu.CompilerParams(
            collective_id=0, has_side_effects=True, vmem_limit_bytes=56 * 1024 * 1024
        ),
        cost_estimate=pl.CostEstimate(
            flops=2 * rows * count * wide * (cells + targets),
            bytes_accessed=2 * blocks.size + 2 * source_state.size,
            transcendentals=0,
        ),
    )(intersection, index_map, source_state, blocks, bracket, fraction)
    return pl.pallas_call(
        store_kernel,
        name="store",
        out_shape=jax.ShapeDtypeStruct(held.shape, bf16),
        in_specs=[pl.BlockSpec(memory_space=pltpu.VMEM)],
        out_specs=pl.BlockSpec(memory_space=pltpu.HBM),
        scratch_shapes=[dma],
        compiler_params=pltpu.CompilerParams(vmem_limit_bytes=8 * 1024 * 1024),
    )(held)


def solution(mesh):
    in_specs = (
        P(None, "lev", "horiz"),
        P("horiz"),
        P("horiz", None),
        P("horiz", None, None),
        P(None, ("horiz", "lev")),
        P(None, ("horiz", "lev")),
    )
    out_specs = P(None, None, ("horiz", "lev"))
    body = functools.partial(local, mesh.shape["lev"], mesh.shape["horiz"])
    return jax.shard_map(body, mesh=mesh, in_specs=in_specs, out_specs=out_specs, check_vma=False)
```

```python
import functools

import jax
import jax.numpy as jnp
from jax import lax
from jax.experimental import pallas as pl
from jax.experimental.pallas import tpu as pltpu
from jax.sharding import PartitionSpec as P

MESH = pl.DeviceIdType.MESH
HIGH = 256
LANES = 128


def round_up(value, step):
    return (value + step - 1) // step * step


def row_plan(fields, slab_levels):
    whole = slab_levels // 16 * 16
    rest = slab_levels - whole
    extra = round_up(fields * rest, 8)
    base = round_up(extra, 16)
    return whole, rest, extra, base, base + fields * whole


def field_groups(fields):
    first = max(1, fields // 5)
    cuts = [0, first, 2 * first, fields - first, fields]
    return [(a, b) for a, b in zip(cuts[:-1], cuts[1:]) if b > a]


def rows_at(table, index):
    numbers = lax.GatherDimensionNumbers(
        offset_dims=(),
        collapsed_slice_dims=(0,),
        start_index_map=(0,),
        operand_batching_dims=(1,),
        start_indices_batching_dims=(1,),
    )
    return lax.gather(
        table, index[..., None], numbers, slice_sizes=(1, 1), mode=lax.GatherScatterMode.PROMISE_IN_BOUNDS
    )


def regrid_kernel(
    groups, levs, depth,
    inter_hbm, index_hbm, source_hbm, blocks_hbm, bracket_hbm, fraction_hbm, out_ref,
    inter_ref, index_ref, tile, spare, first_rows, other_rows, weights, request, wanted, chosen, arrived, total, slab, got,
    brackets, fractions, raw, table,
    inter_sem, index_sem, tile_sem, weight_sem, bracket_sem, fraction_sem,
    req_send, req_recv, val_send, val_recv, lev_send, lev_recv, all_above,
):
    fields, slab_levels, cells = tile.shape
    whole, rest, extra, base, rows = row_plan(fields, slab_levels)
    count = 2 * depth + 1
    wide = index_ref.shape[1]
    me = lax.axis_index("horiz")
    my_lev = lax.axis_index("lev")
    levels_out, columns = brackets.shape
    plan = field_groups(fields)
    chunks = [(base + a * whole, (b - a) * whole) for a, b in plan]
    parts = [[i] for i in range(len(chunks))]
    spans = list(chunks)
    if extra:
        parts[0].append(len(chunks))
        spans[0] = (0, base + chunks[0][1])
        chunks.append((0, extra))

    barrier = pltpu.get_barrier_semaphore()
    offsets = [o for o in range(-depth, depth + 1) if o != 0]
    for offset in offsets:
        pl.semaphore_signal(
            barrier, inc=1, device_id={"horiz": lax.rem(me + offset + groups, groups)}, device_id_type=MESH
        )
    has_below, has_above = my_lev > 0, my_lev < levs - 1

    def tell(semaphore, lev):
        pl.semaphore_signal(semaphore, inc=1, device_id={"lev": lev}, device_id_type=MESH)

    for hop in range(1, levs):
        pl.when(my_lev + hop < levs)(functools.partial(tell, barrier, my_lev + hop))
    greeted = len(offsets) + my_lev

    inter_copy = pltpu.make_async_copy(inter_hbm, inter_ref, inter_sem)
    inter_copy.start()
    index_copy = pltpu.make_async_copy(index_hbm, index_ref, index_sem)
    index_copy.start()
    tile_copy = pltpu.make_async_copy(source_hbm, tile, tile_sem)
    tile_copy.start()
    for part in range(levs):
        copy = pltpu.make_async_copy(
            blocks_hbm.at[:, :, pl.ds(part * columns, columns)], weights.at[:, part], weight_sem
        )
        copy.start()
    bracket_copy = pltpu.make_async_copy(bracket_hbm, brackets, bracket_sem)
    bracket_copy.start()
    fraction_copy = pltpu.make_async_copy(fraction_hbm, fractions, fraction_sem)
    fraction_copy.start()
    inter_copy.wait()
    index_copy.wait()
    slots = []
    for place in range(count):
        group = lax.rem(me + place - depth + groups, groups)
        cells_wanted = jnp.zeros((1, wide), jnp.int32)
        slot = jnp.int32(0)
        for k in range(count):
            hit = (inter_ref[k] == group).astype(jnp.int32)
            cells_wanted = cells_wanted + index_ref[k : k + 1, :] * hit
            slot = jnp.where(inter_ref[k] == group, jnp.int32(k), slot)
        slots.append(slot)
        if place == depth:
            wanted[place] = cells_wanted
        else:
            request[place] = cells_wanted

    def request_copy(place):
        return pltpu.make_async_remote_copy(
            src_ref=request.at[place],
            dst_ref=wanted.at[2 * depth - place],
            send_sem=req_send,
            recv_sem=req_recv.at[2 * depth - place],
            device_id={"horiz": lax.rem(me + place - depth + groups, groups)},
            device_id_type=MESH,
        )

    def value_copy(place, piece, sign):
        first, size = chunks[piece]
        return pltpu.make_async_remote_copy(
            src_ref=chosen.at[place, pl.ds(first, size)],
            dst_ref=arrived.at[2 * depth - place, pl.ds(first, size)],
            send_sem=val_send,
            recv_sem=val_recv.at[sign],
            device_id={"horiz": lax.rem(me + place - depth + groups, groups)},
            device_id_type=MESH,
        )

    def tally(ref, send_sem, recv_sem):
        return pltpu.make_async_remote_copy(
            src_ref=ref,
            dst_ref=ref,
            send_sem=send_sem,
            recv_sem=recv_sem,
            device_id={"lev": dest_of(0)},
            device_id_type=MESH,
        )

    weight_of = [sum(chunks[piece][1] for piece in part) for part in parts]
    sent_rows = sum(weight_of)

    upper = 2 * my_lev >= levs

    def dest_of(turn):
        return turn + (turn >= my_lev).astype(jnp.int32)

    sides = [(0, columns // 2), (columns // 2, columns // 2)]

    def lev_copies(turn, number):
        spread = sides if number == len(parts) - 1 else [(0, columns)]
        return [
            lev_copy(turn, number + side, piece, pl.ds(*lane))
            for side, lane in enumerate(spread)
            for piece in parts[number]
        ]

    def lev_copy(turn, number, piece, lane):
        block = pl.ds(*chunks[piece])
        return pltpu.make_async_remote_copy(
            src_ref=slab.at[turn, block, lane],
            dst_ref=got.at[my_lev, block, lane],
            send_sem=lev_send,
            recv_sem=lev_recv.at[number],
            device_id={"lev": dest_of(turn)},
            device_id_type=MESH,
        )

    pl.semaphore_wait(barrier, greeted)
    pl.when((my_lev == levs - 1) & has_below)(lambda: tell(all_above, my_lev - 1))
    for reach in range(depth, 0, -1):
        request_copy(depth - reach).start()
        request_copy(depth + reach).start()

    tile_copy.wait()
    high_count = cells // HIGH
    head = spans[0][1]
    tail = rows - head
    if base:
        spare[...] = jnp.zeros(spare.shape, jnp.float32)
        for field in range(fields):
            if rest:
                spare[pl.ds(field * rest, rest), :] = tile[field, pl.ds(whole, rest), :].astype(jnp.float32)
    for chunk in range(high_count):
        lane = pl.ds(chunk * HIGH, HIGH)
        if base:
            first_rows[pl.ds(chunk * head, base), :] = spare[:, lane].astype(jnp.bfloat16)
        for field in range(fields):
            if field < plan[0][1]:
                spot = first_rows.at[pl.ds(chunk * head + base + field * whole, whole)]
            else:
                spot = other_rows.at[pl.ds(chunk * tail + base + field * whole - head, whole)]
            spot[...] = tile[field, pl.ds(0, whole), lane]

    ids = lax.broadcasted_iota(jnp.int32, (HIGH, 1), 0).astype(jnp.float32).astype(jnp.bfloat16)

    def select(place, held):
        cell = wanted[place]
        high = cell // HIGH
        low = (cell - high * HIGH).astype(jnp.float32).astype(jnp.bfloat16)
        picker = jnp.where(ids == low, jnp.bfloat16(1), jnp.bfloat16(0))
        found = jnp.dot(held[...], picker, preferred_element_type=jnp.float32)
        size = held.shape[0] // high_count
        values = jnp.zeros((size, wide), jnp.float32)
        for chunk in range(high_count):
            values = jnp.where(high == chunk, found[chunk * size : (chunk + 1) * size], values)
        return values.astype(jnp.bfloat16)

    first_span, other_span = pl.ds(0, head), pl.ds(head, tail)
    arrived[depth, first_span] = select(depth, first_rows)
    arrived[depth, other_span] = select(depth, other_rows)

    def hand_down():
        pl.semaphore_wait(all_above, 1)
        tell(all_above, my_lev - 1)

    between = has_below & has_above
    pl.when(between & upper)(hand_down)

    lean = 1 - 2 * (me % 2)

    def order_place(step):
        reach = depth - step // 2
        return depth + reach * (2 * (step % 2) - 1) * lean

    last = 2 * depth - 1

    near = order_place(last)
    request_copy(2 * depth - near).wait_recv()
    chosen[near, first_span] = select(near, first_rows)
    chosen[near, other_span] = select(near, other_rows)
    for piece in range(len(chunks)):
        value_copy(near, piece, len(parts)).start()

    def serve(step, carry):
        place = order_place(step)
        request_copy(2 * depth - place).wait_recv()
        chosen[place, first_span] = select(place, first_rows)
        for piece in parts[0]:
            value_copy(place, piece, 0).start()
        return carry

    lax.fori_loop(0, last, serve, 0)

    pl.when(between & jnp.logical_not(upper))(hand_down)

    def serve_rest(step, carry):
        place = order_place(step)
        chosen[place, other_span] = select(place, other_rows)
        for piece in parts[1]:
            value_copy(place, piece, 1).start()
        return carry

    lax.fori_loop(0, last, serve_rest, 0)
    for later in range(2, len(parts)):
        for step in range(last):
            for piece in parts[later]:
                value_copy(order_place(step), piece, later).start()
    pltpu.make_async_copy(weights, weights, weight_sem).wait()

    def slot_of(place):
        slot = slots[0]
        for k in range(1, count):
            slot = jnp.where(place == k, slots[k], slot)
        return slot

    tally(arrived.at[0, pl.ds(0, sent_rows)], val_send, val_recv.at[len(parts)]).wait_recv()
    beside = [(arrived[depth], slots[depth]), (arrived[near], slot_of(near))]
    for part in range(levs):
        total[part] = sum(
            jnp.dot(value, weights[slot, part], preferred_element_type=jnp.float32) for value, slot in beside
        )

    def send_others(number):
        for turn in range(1, levs - 1):
            for copy in lev_copies(turn, number):
                copy.start()

    if levs > 1:
        pl.when(my_lev == 0)(lambda: pl.semaphore_wait(all_above, 1))
    far = [order_place(step) for step in range(last)]
    far_slots = [slot_of(place) for place in far]
    for number in range(len(parts)):
        tally(arrived.at[pl.ds(0, last), pl.ds(0, weight_of[number])], val_send, val_recv.at[number]).wait_recv()

        def column_sum(part, block, values, lane=pl.ds(0, columns)):
            sums = total[part, block, lane]
            for value, slot in zip(values, far_slots):
                sums += jnp.dot(value, weights[slot, part, :, lane], preferred_element_type=jnp.float32)
            return sums.astype(jnp.bfloat16)

        block = pl.ds(*spans[number])
        values = [arrived[place, block] for place in far]
        copies = lev_copies(0, number)
        if number == len(parts) - 1:
            for side, copy in zip(sides, copies):
                lane = pl.ds(*side)
                slab[0, block, lane] = column_sum(dest_of(0), block, values, lane)
                copy.start()
        else:
            slab[0, block] = column_sum(dest_of(0), block, values)
            for copy in copies:
                copy.start()
        if number == len(parts) - 2:
            continue
        members = [number]
        if number == len(parts) - 1:
            pl.when(upper)(functools.partial(send_others, len(parts) - 3))
            members = [number - 1, number]
            block = pl.ds(spans[number - 1][0], spans[number - 1][1] + spans[number][1])
            values = [arrived[place, block] for place in far]
        for turn in range(1, levs - 1):
            slab[turn, block] = column_sum(dest_of(turn), block, values)
        got[my_lev, block] = column_sum(my_lev, block, values)
        for member in members:
            if member != len(parts) - 3:
                send_others(member)
            else:
                pl.when(jnp.logical_not(upper))(functools.partial(send_others, member))

    bracket_copy.wait()
    fraction_copy.wait()
    levels_in = levs * slab_levels
    step_rows = 16
    table[:, pl.ds(levels_in, table.shape[1] - levels_in), :] = jnp.zeros(
        (table.shape[0], table.shape[1] - levels_in, LANES), jnp.float32
    )

    def interpolate(first, end, low_strip, high_strip):
        held = list(range(first, end))

        def work(strip, carry):
            lane = pl.ds(pl.multiple_of(strip * LANES, LANES), LANES)
            for lev in range(levs):
                if rest:
                    raw[lev] = got[lev, pl.ds(0, base), lane].astype(jnp.float32)
                for place, field in enumerate(held):
                    table[place, pl.ds(lev * slab_levels, whole), :] = got[
                        lev, pl.ds(base + field * whole, whole), lane
                    ].astype(jnp.float32)
                    if rest:
                        table[place, pl.ds(lev * slab_levels + whole, rest), :] = raw[
                            lev, pl.ds(field * rest, rest), :
                        ]
            for start in range(0, levels_out, step_rows):
                size = min(step_rows, levels_out - start)
                bracket = brackets[start : start + size, lane]
                upper = fractions[start : start + size, lane]
                if size < step_rows:
                    bracket = jnp.concatenate([bracket, jnp.zeros((step_rows - size, LANES), jnp.int32)], axis=0)
                    upper = jnp.concatenate([upper, jnp.zeros((step_rows - size, LANES), jnp.float32)], axis=0)
                halves = [bracket[i : i + 8] for i in range(0, step_rows, 8)]
                high = [half >> 3 for half in halves]
                low = [half & 7 for half in halves]
                counts = (levels_in - 2) // 8 + 1
                bits = max(1, (counts - 1).bit_length())
                turns = [[(h & (1 << bit)) != 0 for bit in range(bits)] for h in high]

                def choose(place, first, size, i):
                    if size == 1:
                        here = table[place, pl.ds(first * 8, 8), :]
                        over = table[place, pl.ds(first * 8 + 1, 8), :]
                        return rows_at(here, low[i]), rows_at(over, low[i])
                    half = size // 2
                    left = choose(place, first, half, i)
                    if first + half >= counts:
                        return left
                    right = choose(place, first + half, half, i)
                    mask = turns[i][half.bit_length() - 1]
                    return tuple(jnp.where(mask, b, a) for a, b in zip(left, right))

                below = [[None] * len(halves) for _ in held]
                above = [[None] * len(halves) for _ in held]
                for place in range(len(held)):
                    for i in range(len(halves)):
                        below[place][i], above[place][i] = choose(place, 0, 1 << bits, i)
                for place, field in enumerate(held):
                    mixed = (1.0 - upper) * jnp.concatenate(below[place], axis=0) + upper * jnp.concatenate(
                        above[place], axis=0
                    )
                    out_ref[field, start : start + size, lane] = mixed[:size].astype(jnp.bfloat16)
            return carry

        lax.fori_loop(low_strip, high_strip, work, 0)

    for number, (first, end) in enumerate(plan):
        for side, (left, width) in enumerate(sides if number == len(parts) - 1 else [(0, columns)]):
            landed = got.at[pl.ds(0, levs - 1), pl.ds(0, weight_of[number]), pl.ds(0, width)]
            tally(landed, lev_send, lev_recv.at[number + side]).wait_recv()
            interpolate(first, end, left // LANES, (left + width) // LANES)

    tally(slab.at[:, pl.ds(0, sent_rows)], lev_send, lev_recv.at[0]).wait_send()
    tally(chosen.at[pl.ds(0, 2 * depth), pl.ds(0, sent_rows)], val_send, val_recv.at[0]).wait_send()
    tally(request.at[pl.ds(0, 2 * depth)], req_send, req_recv.at[0]).wait_send()


def store_kernel(held_ref, out_hbm, sem):
    copies = [
        pltpu.make_async_copy(held_ref, out_hbm, sem)
    ]
    for copy in copies:
        copy.start()
    for copy in copies:
        copy.wait()


def local(levs, groups, source_state, intersection, index_map, blocks, bracket, fraction):
    fields, slab_levels, cells = source_state.shape
    count, wide, targets = blocks.shape
    depth = (count - 1) // 2
    whole, rest, extra, base, rows = row_plan(fields, slab_levels)
    columns = targets // levs
    levels_out = bracket.shape[0]
    plan = field_groups(fields)
    most = max(b - a for a, b in plan)
    head = base + plan[0][1] * whole
    bf16, f32, i32 = jnp.bfloat16, jnp.float32, jnp.int32
    dma = pltpu.SemaphoreType.DMA
    held = pl.pallas_call(
        functools.partial(regrid_kernel, groups, levs, depth),
        name="regrid",
        out_shape=pltpu.VMEM((fields, levels_out, columns), bf16),
        in_specs=[pl.BlockSpec(memory_space=pltpu.HBM)] * 6,
        out_specs=pl.BlockSpec(memory_space=pltpu.VMEM),
        scratch_shapes=[
            pltpu.SMEM((count,), i32),
            pltpu.VMEM((count, wide), i32),
            pltpu.VMEM((fields, slab_levels, cells), bf16),
            pltpu.VMEM((max(base, 8), cells), f32),
            pltpu.VMEM((cells // HIGH * head, HIGH), bf16),
            pltpu.VMEM((cells // HIGH * (rows - head), HIGH), bf16),
            pltpu.VMEM((count, levs, wide, columns), bf16),
            pltpu.VMEM((count, 1, wide), i32),
            pltpu.VMEM((count, 1, wide), i32),
            pltpu.VMEM((count, rows, wide), bf16),
            pltpu.VMEM((count, rows, wide), bf16),
            pltpu.VMEM((levs, rows, columns), f32),
            pltpu.VMEM((levs - 1, rows, columns), bf16),
            pltpu.VMEM((levs, rows, columns), bf16),
            pltpu.VMEM((levels_out, columns), i32),
            pltpu.VMEM((levels_out, columns), f32),
            pltpu.VMEM((levs, max(base, 8), LANES), f32),
            pltpu.VMEM((most, round_up(levs * slab_levels, 8) + 8, LANES), f32),
            dma,
            dma,
            dma,
            dma,
            dma,
            dma,
            dma,
            dma((count,)),
            dma,
            dma((len(plan) + 1,)),
            dma,
            dma((len(plan) + 1,)),
            pltpu.SemaphoreType.REGULAR,
        ],
        compiler_params=pltpu.CompilerParams(
            collective_id=0, has_side_effects=True, vmem_limit_bytes=56 * 1024 * 1024
        ),
        cost_estimate=pl.CostEstimate(
            flops=2 * rows * count * wide * (cells + targets),
            bytes_accessed=2 * blocks.size + 2 * source_state.size,
            transcendentals=0,
        ),
    )(intersection, index_map, source_state, blocks, bracket, fraction)
    return pl.pallas_call(
        store_kernel,
        name="store",
        out_shape=jax.ShapeDtypeStruct(held.shape, bf16),
        in_specs=[pl.BlockSpec(memory_space=pltpu.VMEM)],
        out_specs=pl.BlockSpec(memory_space=pltpu.HBM),
        scratch_shapes=[dma],
        compiler_params=pltpu.CompilerParams(vmem_limit_bytes=8 * 1024 * 1024),
    )(held)


def solution(mesh):
    in_specs = (
        P(None, "lev", "horiz"),
        P("horiz"),
        P("horiz", None),
        P("horiz", None, None),
        P(None, ("horiz", "lev")),
        P(None, ("horiz", "lev")),
    )
    out_specs = P(None, None, ("horiz", "lev"))
    body = functools.partial(local, mesh.shape["lev"], mesh.shape["horiz"])
    return jax.shard_map(body, mesh=mesh, in_specs=in_specs, out_specs=out_specs, check_vma=False)
```
